8 devices in a mesh: pod: 1 (over z), dp: 2 (over y), sp: 4 (over x, core).
Axes of the slice: x: 2, y: 2, z: 1, core: 2. Of those that a mesh axis runs over, the one named last changes fastest.
Arguments:
- images: bfloat16 [32, 48, 168, 128], P(('pod', 'dp'), 'sp')
- w_a: bfloat16 [2, 3, 3, 128, 128], replicated
- norm_a: float32 [2, 2, 128], replicated
- w_down: bfloat16 [3, 3, 128, 256], replicated
- norm_down: float32 [2, 256], replicated
- w_b: bfloat16 [1, 3, 3, 256, 256], replicated
- norm_b: float32 [1, 2, 256], replicated
Outputs:
- output: bfloat16 [32, 24, 84, 256], P(('pod', 'dp'), 'sp')
All inputs are finite; a program needn't handle non-finite values.
Results may differ from the reference program's by a relative error of at most 0.00496.
Values are sent between devices in bfloat16 or wider.
A program may use at most 1 GiB of HBM per device.

```python
import jax
import jax.numpy as jnp
from jax import lax

BATCH = 32
HEIGHT = 48
WIDTH = 168
CH_A = 128
CH_B = 256
LAYERS_A = 2
LAYERS_B = 1
EPS_VALUE = 1e-5
CONV_DIMS = ('NHWC', 'HWIO', 'NHWC')


def setup_inputs(seed: int = 0, part: int = 0) -> dict:
    base_key = jax.random.key(seed)
    part_key = jax.random.fold_in(base_key, part)
    noise_key, dir_key, scale_key, offset_key, phase_key = jax.random.split(part_key, 5)
    weight_keys = jax.random.split(base_key, 9)
    row_pos = jnp.arange(HEIGHT, dtype=jnp.float32) * (2.0 / (HEIGHT - 1)) - 1.0
    row_col = row_pos[None, :, None, None]
    noise = jax.random.normal(noise_key, (BATCH, HEIGHT, WIDTH, CH_A), jnp.float32)
    chan_dir = jax.random.normal(dir_key, (BATCH, 1, 1, CH_A), jnp.float32)
    img_scale = jax.random.uniform(scale_key, (BATCH, 1, 1, 1), jnp.float32, 0.5, 1.5)
    img_offset = 0.5 * jax.random.normal(offset_key, (BATCH, 1, 1, CH_A), jnp.float32)
    phase = jax.random.uniform(phase_key, (BATCH, 1, 1, CH_A), jnp.float32, 0.0, 6.2831853)
    wave = 0.5 * jnp.sin(row_col * 7.0 + phase)
    x_val = img_scale * (0.7 * noise + row_col * chan_dir + wave) + img_offset
    w_a = jax.random.normal(weight_keys[0], (LAYERS_A, 3, 3, CH_A, CH_A), jnp.float32) * (9 * CH_A) ** -0.5
    norm_a = jnp.stack([jax.random.uniform(weight_keys[1], (LAYERS_A, CH_A), jnp.float32, 0.6, 1.4), 0.3 * jax.random.normal(weight_keys[2], (LAYERS_A, CH_A), jnp.float32)], axis=1)
    w_down = jax.random.normal(weight_keys[3], (3, 3, CH_A, CH_B), jnp.float32) * (9 * CH_A) ** -0.5
    norm_down = jnp.stack([jax.random.uniform(weight_keys[4], (CH_B,), jnp.float32, 0.6, 1.4), 0.3 * jax.random.normal(weight_keys[5], (CH_B,), jnp.float32)])
    w_b = jax.random.normal(weight_keys[6], (LAYERS_B, 3, 3, CH_B, CH_B), jnp.float32) * (9 * CH_B) ** -0.5
    norm_b = jnp.stack([jax.random.uniform(weight_keys[7], (LAYERS_B, CH_B), jnp.float32, 0.6, 1.4), 0.3 * jax.random.normal(weight_keys[8], (LAYERS_B, CH_B), jnp.float32)], axis=1)
    return {'images': x_val.astype(jnp.bfloat16), 'w_a': w_a.astype(jnp.bfloat16), 'norm_a': norm_a, 'w_down': w_down.astype(jnp.bfloat16), 'norm_down': norm_down, 'w_b': w_b.astype(jnp.bfloat16), 'norm_b': norm_b}


def conv_norm(hidden, weight, norm_pair, stride, pads):
    z_val = lax.conv_general_dilated(hidden.astype(jnp.float32), weight.astype(jnp.float32), (stride, stride), pads, dimension_numbers=CONV_DIMS)
    mean_val = jnp.mean(z_val, axis=(0, 1, 2))
    mean_sq = jnp.mean(z_val * z_val, axis=(0, 1, 2))
    inv_std = lax.rsqrt(mean_sq - mean_val * mean_val + EPS_VALUE)
    scaled = norm_pair[0] * (z_val - mean_val) * inv_std + norm_pair[1]
    return jnp.maximum(scaled, 0.0).astype(jnp.bfloat16)


def reference(images, w_a, norm_a, w_down, norm_down, w_b, norm_b):
    def same_step(hidden, layer_args):
        return conv_norm(hidden, layer_args[0], layer_args[1], 1, ((1, 1), (1, 1))), None
    hidden, unused_a = lax.scan(same_step, images, (w_a, norm_a))
    hidden = conv_norm(hidden, w_down, norm_down, 2, ((0, 1), (0, 1)))
    hidden, unused_b = lax.scan(same_step, hidden, (w_b, norm_b))
    return hidden
```

```python
import functools

import jax
import jax.numpy as jnp
from jax import lax
from jax.experimental import pallas as pl
from jax.experimental.pallas import tpu as pltpu
from jax.sharding import PartitionSpec as P

EPS_VALUE = 1e-5
F32 = jnp.float32
BF16 = jnp.bfloat16
MESH = pl.DeviceIdType.MESH

NIM = 16
ROWS = 12
COLS = 168
HALF = COLS // 2
MROW = HALF * NIM
YROW = (HALF + 1) * NIM
OROWS = 6
OCOLS = 84
OROW = OCOLS * NIM
O3ROW = (OCOLS + 2) * NIM
CHUNK = 336
GROUPS = 8


def kernel(x_ref, wa_ref, na_ref, wd_ref, nd_ref, wb_ref, nb_ref, out_ref,
           xs, tr, yy, zz, y3, z3, yo, wraw, wt, wdv, wbv, nav, ndv, nbv,
           st_out, st_in,
           x_sem, w_sem, xh_send, xh_recv, h2_send, h2_recv, h3_send, h3_recv, h4_send, h4_recv,
           st_send, st_recv, o_sem):
    dp = lax.axis_index("dp")
    sp = lax.axis_index("sp")
    me = dp * 4 + sp

    def x_copy(r):
        return pltpu.make_async_copy(x_ref.at[:, r], xs.at[r + 1], x_sem.at[r])
    w_copies = [
        pltpu.make_async_copy(wa_ref, wraw, w_sem.at[0]),
        pltpu.make_async_copy(wd_ref, wdv, w_sem.at[1]),
        pltpu.make_async_copy(wb_ref, wbv, w_sem.at[2]),
        pltpu.make_async_copy(na_ref, nav, w_sem.at[3]),
        pltpu.make_async_copy(nd_ref, ndv, w_sem.at[4]),
        pltpu.make_async_copy(nb_ref, nbv, w_sem.at[5]),
    ]
    w_copies[0].start()
    for r in (1, 2, 3, 4, 5, 6, 7, 8, 9, 10, 0, 11):
        x_copy(r).start()
    for c in w_copies[1:]:
        c.start()

    barrier = pltpu.get_barrier_semaphore()

    def peer(k):
        other = lax.rem(me + k, GROUPS)
        return (0, other // 4, lax.rem(other, 4))
    for k in range(1, GROUPS):
        pl.semaphore_signal(barrier, inc=1, device_id=peer(k), device_id_type=MESH)
    pl.semaphore_wait(barrier, GROUPS - 1)

    up = (0, dp, lax.rem(sp + 3, 4))
    down = (0, dp, lax.rem(sp + 1, 4))
    has_up = sp > 0
    has_down = sp < 3

    def halo(src_hi, dst_hi, src_lo, dst_lo, send, recv):
        hi = None if src_hi is None else pltpu.make_async_remote_copy(
            src_ref=src_hi, dst_ref=dst_hi, send_sem=send.at[0], recv_sem=recv.at[0],
            device_id=up, device_id_type=MESH)
        lo = None if src_lo is None else pltpu.make_async_remote_copy(
            src_ref=src_lo, dst_ref=dst_lo, send_sem=send.at[1], recv_sem=recv.at[1],
            device_id=down, device_id_type=MESH)

        def start():
            if hi is not None:
                @pl.when(has_up)
                def _():
                    hi.start()
            if lo is not None:
                @pl.when(has_down)
                def _():
                    lo.start()

        def wait_send():
            if hi is not None:
                @pl.when(has_up)
                def _():
                    hi.wait_send()
            if lo is not None:
                @pl.when(has_down)
                def _():
                    lo.wait_send()

        def wait_recv():
            if hi is not None:
                @pl.when(has_down)
                def _():
                    hi.wait_recv()
            if lo is not None:
                @pl.when(has_up)
                def _():
                    lo.wait_recv()
        return start, wait_send, wait_recv

    xh = halo(x_ref.at[:, 0], xs.at[ROWS + 1], x_ref.at[:, ROWS - 1], xs.at[0], xh_send, xh_recv)
    h2 = halo(yy.at[:, 1], yy.at[:, ROWS + 1], yy.at[:, ROWS], yy.at[:, 0], h2_send, h2_recv)
    h3 = halo(yy.at[:, 1], yy.at[:, ROWS + 1], None, None, h3_send, h3_recv)
    h4 = halo(y3.at[1], y3.at[OROWS + 1], y3.at[OROWS], y3.at[0], h4_send, h4_recv)

    xh[0]()

    zpad = jnp.zeros((NIM, 128), BF16)

    @pl.loop(0, ROWS + 2)
    def _(r):
        yy[0, r, pl.ds(0, NIM), :] = zpad
        yy[1, r, pl.ds(HALF * NIM, NIM), :] = zpad

    @pl.loop(0, OROWS + 2)
    def _(r):
        for c in (0, OCOLS + 1):
            y3[r, pl.ds(c * NIM, NIM), :] = jnp.zeros((NIM, 256), BF16)

    @pl.when(sp == 0)
    def _():
        for b in range(2):
            yy[b, 0] = jnp.zeros((YROW, 128), BF16)
        y3[0] = jnp.zeros((O3ROW, 256), BF16)

    @pl.when(sp == 3)
    def _():
        for b in range(2):
            yy[b, ROWS + 1] = jnp.zeros((YROW, 128), BF16)
        y3[OROWS + 1] = jnp.zeros((O3ROW, 256), BF16)

    w_copies[0].wait()
    zblk = jnp.zeros((128, 128), BF16)
    for layer in range(2):
        for q in range(3):
            k = 256 * q
            wt[layer, pl.ds(k, 128), pl.ds(0, 128)] = wraw[layer, 1, q]
            wt[layer, pl.ds(k, 128), pl.ds(128, 128)] = wraw[layer, 0, q]
            wt[layer, pl.ds(k + 128, 128), pl.ds(0, 128)] = wraw[layer, 2, q]
            wt[layer, pl.ds(k + 128, 128), pl.ds(128, 128)] = wraw[layer, 1, q]
            k = 768 + 256 * q
            wt[layer, pl.ds(k, 128), pl.ds(0, 128)] = wraw[layer, 0, q]
            wt[layer, pl.ds(k, 128), pl.ds(128, 128)] = zblk
            wt[layer, pl.ds(k + 128, 128), pl.ds(0, 128)] = zblk
            wt[layer, pl.ds(k + 128, 128), pl.ds(128, 128)] = wraw[layer, 2, q]
    for c in w_copies[1:]:
        c.wait()

    def transpose_row(r):
        for n in range(NIM):
            tr[pl.ds(n * COLS, COLS), :] = xs[r, n].astype(F32)
        for j in range(COLS):
            v = tr[pl.ds(j, NIM, stride=COLS), :].astype(BF16)
            b, a = (j + 1) % 2, (j + 1) // 2
            yy[b, r, pl.ds(a * NIM, NIM), :] = v

    def transpose_own(r):
        x_copy(r).wait()
        transpose_row(r + 1)

    @pl.loop(0, ROWS)
    def _(r):
        transpose_own(r)

    def exchange(layer, rows):
        buf = jnp.concatenate(rows + [jnp.zeros((8 - len(rows), 128), F32)], axis=0)
        st_out[layer] = buf
        st_in[layer, me] = buf
        copies = []
        for k in range(1, GROUPS):
            copies.append(pltpu.make_async_remote_copy(
                src_ref=st_out.at[layer], dst_ref=st_in.at[layer, me],
                send_sem=st_send.at[layer, k], recv_sem=st_recv.at[layer, k],
                device_id=peer(k), device_id_type=MESH))
        for c in copies:
            c.start()
        for c in copies:
            c.wait_recv()
        total = st_in[layer, 0]
        for s in range(1, GROUPS):
            total = total + st_in[layer, s]

        def finish():
            for c in copies:
                c.wait_send()
        return total, finish

    def moments(s1, s2, count):
        mean = s1 / count
        var = s2 / count - mean * mean
        return mean, lax.rsqrt(var + EPS_VALUE)

    def normalise(z, mean, inv, gamma, beta):
        return jnp.maximum(gamma * (z - mean) * inv + beta, 0.0).astype(BF16)

    TAPS = (((0, 0), (1, 0), (0, NIM)), ((1, 0), (0, NIM), (1, NIM)))

    def pair_layer(layer, before_border):
        def body(it, carry):
            s1, s2 = carry
            pair = jnp.where(it < 4, it + 1, (it - 4) * 5)
            i = pair * 2

            @pl.when(it == 4)
            def _():
                before_border()
            for b in range(2):
                for m in range(0, MROW, CHUNK):
                    parts = []
                    for rows in ((1, 2), (0, 3)):
                        for plane, off in TAPS[b]:
                            for rr in rows:
                                parts.append(yy[plane, i + rr, pl.ds(m + off, CHUNK), :])
                    lhs = jnp.concatenate(parts, axis=1)
                    res = jnp.dot(lhs, wt[layer], preferred_element_type=F32)
                    zz[b, i, pl.ds(m, CHUNK), :] = res[:, :128]
                    zz[b, i + 1, pl.ds(m, CHUNK), :] = res[:, 128:]
                    r3 = res.reshape(CHUNK // 8, 8, 256)
                    s1 = s1 + jnp.sum(r3, axis=0)
                    s2 = s2 + jnp.sum(r3 * r3, axis=0)
            return s1, s2
        zero = jnp.zeros((8, 256), F32)
        s1, s2 = lax.fori_loop(0, ROWS // 2, body, (zero, zero))
        s1 = jnp.sum(s1, axis=0, keepdims=True)
        s2 = jnp.sum(s2, axis=0, keepdims=True)
        total, finish = exchange(layer, [s1[:, :128] + s1[:, 128:], s2[:, :128] + s2[:, 128:]])
        mean, inv = moments(total[0:1], total[1:2], float(32 * 48 * 168))
        return mean, inv, finish

    def norm_row(r, mean, inv, gamma, beta):
        yy[1, r + 1, pl.ds(0, MROW), :] = normalise(zz[0, r], mean, inv, gamma, beta)
        yy[0, r + 1, pl.ds(NIM, MROW), :] = normalise(zz[1, r], mean, inv, gamma, beta)

    def first_border():
        xh[2]()

        @pl.when(has_up)
        def _():
            transpose_row(0)

        @pl.when(has_down)
        def _():
            transpose_row(ROWS + 1)

    mean, inv, fin1 = pair_layer(0, first_border)
    gamma, beta = nav[0, 0:1], nav[0, 1:2]

    @pl.loop(0, 2)
    def _(e):
        norm_row(e * (ROWS - 1), mean, inv, gamma, beta)
    h2[0]()

    @pl.loop(1, ROWS - 1)
    def _(r):
        norm_row(r, mean, inv, gamma, beta)

    mean2, inv2, fin2 = pair_layer(1, h2[2])
    gamma2, beta2 = nav[1, 0:1], nav[1, 1:2]
    h2[1]()
    norm_row(0, mean2, inv2, gamma2, beta2)
    h3[0]()

    @pl.loop(1, ROWS)
    def _(r):
        norm_row(r, mean2, inv2, gamma2, beta2)

    wd_taps = ((1, 0), (0, NIM), (1, NIM))

    def wide_layer(layer, n_it, row_of, lhs_of, w_val, before_last):
        def body(it, carry):
            s1, s2 = carry
            i = row_of(it)
            before_last(it)
            for m in range(0, OROW, CHUNK):
                lhs = jnp.concatenate(lhs_of(i, m), axis=1)
                res = jnp.dot(lhs, w_val, preferred_element_type=F32)
                z3[i, pl.ds(m, CHUNK), :] = res
                r3 = res.reshape(CHUNK // 8, 8, 256)
                s1 = s1 + jnp.sum(r3, axis=0)
                s2 = s2 + jnp.sum(r3 * r3, axis=0)
            return s1, s2
        zero = jnp.zeros((8, 256), F32)
        s1, s2 = lax.fori_loop(0, n_it, body, (zero, zero))
        s1 = jnp.sum(s1, axis=0, keepdims=True)
        s2 = jnp.sum(s2, axis=0, keepdims=True)
        total, finish = exchange(layer, [s1[:, :128], s1[:, 128:], s2[:, :128], s2[:, 128:]])
        s1 = jnp.concatenate([total[0:1], total[1:2]], axis=1)
        s2 = jnp.concatenate([total[2:3], total[3:4]], axis=1)
        mean, inv = moments(s1, s2, float(32 * 24 * 84))
        return mean, inv, finish

    def down_lhs(i, m):
        return [yy[plane, 2 * i + p + 1, pl.ds(m + off, CHUNK), :] for p in range(3) for plane, off in wd_taps]

    def down_border(it):
        @pl.when(it == OROWS - 1)
        def _():
            h3[2]()

    mean3, inv3, fin3 = wide_layer(2, OROWS, lambda it: it, down_lhs, wdv[...].reshape(9 * 128, 256), down_border)
    gamma3, beta3 = ndv[0:1], ndv[1:2]

    def norm3(r):
        y3[r + 1, pl.ds(NIM, OROW), :] = normalise(z3[r], mean3, inv3, gamma3, beta3)

    @pl.loop(0, 2)
    def _(e):
        norm3(e * (OROWS - 1))
    h4[0]()

    @pl.loop(1, OROWS - 1)
    def _(r):
        norm3(r)

    def last_lhs(i, m):
        return [y3[i + p, pl.ds(m + NIM * q, CHUNK), :] for p in range(3) for q in range(3)]

    def last_border(it):
        @pl.when(it == OROWS - 2)
        def _():
            h4[2]()

    mean4, inv4, fin4 = wide_layer(
        3, OROWS, lambda it: jnp.where(it < 4, it + 1, (it - 4) * 5), last_lhs,
        wbv[...].reshape(9 * 256, 256), last_border)
    gamma4, beta4 = nbv[0, 0:1], nbv[0, 1:2]

    def o_copy(r):
        return pltpu.make_async_copy(yo.at[r], out_ref.at[r], o_sem.at[r])

    @pl.loop(0, OROWS)
    def _(r):
        yo[r] = normalise(z3[r], mean4, inv4, gamma4, beta4)
        o_copy(r).start()

    xh[1]()
    h3[1]()
    h4[1]()
    for f in (fin1, fin2, fin3, fin4):
        f()

    @pl.loop(0, OROWS)
    def _(r):
        o_copy(r).wait()


def solution(mesh):
    any_spec = pl.BlockSpec(memory_space=pl.ANY)
    dma = pltpu.SemaphoreType.DMA

    def local_stack(images, w_a, norm_a, w_down, norm_down, w_b, norm_b):
        out = pl.pallas_call(
            kernel,
            out_shape=jax.ShapeDtypeStruct((OROWS, OROW, 256), BF16),
            in_specs=[any_spec] * 7,
            out_specs=any_spec,
            scratch_shapes=[
                pltpu.VMEM((ROWS + 2, NIM, COLS, 128), BF16),
                pltpu.VMEM((NIM * COLS, 128), F32),
                pltpu.VMEM((2, ROWS + 2, YROW, 128), BF16),
                pltpu.VMEM((2, ROWS, MROW, 128), F32),
                pltpu.VMEM((OROWS + 2, O3ROW, 256), BF16),
                pltpu.VMEM((OROWS, OROW, 256), F32),
                pltpu.VMEM((OROWS, OROW, 256), BF16),
                pltpu.VMEM((2, 3, 3, 128, 128), BF16),
                pltpu.VMEM((2, 1536, 256), BF16),
                pltpu.VMEM((3, 3, 128, 256), BF16),
                pltpu.VMEM((3, 3, 256, 256), BF16),
                pltpu.VMEM((2, 2, 128), F32),
                pltpu.VMEM((2, 256), F32),
                pltpu.VMEM((1, 2, 256), F32),
                pltpu.VMEM((4, 8, 128), F32),
                pltpu.VMEM((4, GROUPS, 8, 128), F32),
                dma((ROWS,)), dma((6,)),
                dma((2,)), dma((2,)), dma((2,)), dma((2,)), dma((2,)), dma((2,)), dma((2,)), dma((2,)),
                dma((4, GROUPS)), dma((4, GROUPS)), dma((OROWS,)),
            ],
            compiler_params=pltpu.CompilerParams(
                collective_id=0, has_side_effects=True, vmem_limit_bytes=67043328),
        )(images, w_a, norm_a, w_down, norm_down, w_b.reshape(3, 3, 256, 256), norm_b)
        return jnp.transpose(out.reshape(OROWS, OCOLS, NIM, 256), (2, 0, 1, 3))

    act_spec = P(('pod', 'dp'), 'sp', None, None)
    return jax.shard_map(local_stack, mesh=mesh, in_specs=(act_spec, P(), P(), P(), P(), P(), P()), out_specs=act_spec, check_vma=False)
```

```python
import functools

import jax
import jax.numpy as jnp
from jax import lax
from jax.experimental import pallas as pl
from jax.experimental.pallas import tpu as pltpu
from jax.sharding import PartitionSpec as P

EPS_VALUE = 1e-5
F32 = jnp.float32
BF16 = jnp.bfloat16
MESH = pl.DeviceIdType.MESH

NIM = 16
ROWS = 12
COLS = 168
HALF = COLS // 2
MROW = HALF * NIM
YROW = (HALF + 1) * NIM
OROWS = 6
OCOLS = 84
OROW = OCOLS * NIM
O3ROW = (OCOLS + 2) * NIM
CHUNK = 336
VLIM = 59 * 1024 * 1024
GROUPS = 8


def kernel(x_ref, wa_ref, na_ref, wd_ref, nd_ref, wb_ref, nb_ref, out_ref,
           xs, tr, yy, zz, y3, z3, wraw, wt, wdv, wbv, nav, ndv, nbv,
           st_out, st_in,
           x_sem, w_sem, hx_send, hx_recv, h2_send, h2_recv, h3_send, h3_recv, h4_send, h4_recv,
           st_send, st_recv):
    dp = lax.axis_index("dp")
    sp = lax.axis_index("sp")
    me = dp * 4 + sp
    flip = 1 - lax.rem(sp, 2)
    near = (0, dp, sp + 2 * flip - 1)
    far = (0, dp, lax.rem(7 - sp, 4))
    has_far = jnp.logical_or(sp == 1, sp == 2)

    def x_row(r):
        return r + flip * (ROWS - 1 - 2 * r)

    def tap(p):
        return p + flip * (2 - 2 * p)

    def x_copy(r):
        return pltpu.make_async_copy(x_ref.at[:, x_row(r)], xs.at[r + 1], x_sem.at[r])
    wa_copies = [pltpu.make_async_copy(wa_ref.at[l, tap(p)], wraw.at[l, p], w_sem.at[3 * l + p])
                 for l in range(2) for p in range(3)]
    w_copies = [pltpu.make_async_copy(na_ref, nav, w_sem.at[6]),
                pltpu.make_async_copy(nd_ref, ndv, w_sem.at[7]),
                pltpu.make_async_copy(nb_ref, nbv, w_sem.at[8])]
    for p in range(3):
        w_copies.append(pltpu.make_async_copy(wd_ref.at[tap(p)], wdv.at[p], w_sem.at[9 + p]))
        w_copies.append(pltpu.make_async_copy(wb_ref.at[tap(p)], wbv.at[p], w_sem.at[12 + p]))

    barrier = pltpu.get_barrier_semaphore()

    def peer(k):
        other = lax.rem(me + k, GROUPS)
        return (0, other // 4, lax.rem(other, 4))
    for k in range(1, GROUPS):
        pl.semaphore_signal(barrier, inc=1, device_id=peer(k), device_id_type=MESH)

    for r in range(3):
        x_copy(r).start()
    for c in wa_copies:
        c.start()
    for r in range(3, ROWS):
        x_copy(r).start()
    for c in w_copies:
        c.start()

    def halo(src_near, dst_near, src_far, dst_far, send, recv):
        n_copy = pltpu.make_async_remote_copy(
            src_ref=src_near, dst_ref=dst_near, send_sem=send.at[0], recv_sem=recv.at[0],
            device_id=near, device_id_type=MESH)
        f_copy = pltpu.make_async_remote_copy(
            src_ref=src_far, dst_ref=dst_far, send_sem=send.at[1], recv_sem=recv.at[1],
            device_id=far, device_id_type=MESH)
        return n_copy, f_copy

    hx_near, hx_far = halo(x_ref.at[:, x_row(0)], xs.at[0], x_ref.at[:, x_row(ROWS - 1)], xs.at[ROWS + 1],
                           hx_send, hx_recv)
    h2_near, h2_far = halo(yy.at[:, 1], yy.at[:, 0], yy.at[:, ROWS], yy.at[:, ROWS + 1], h2_send, h2_recv)
    h3_near, h3_far = halo(yy.at[:, 1], yy.at[:, 0], yy.at[:, ROWS], yy.at[:, ROWS + 1], h3_send, h3_recv)
    h4_near, h4_far = halo(y3.at[1], y3.at[0], y3.at[OROWS], y3.at[OROWS + 1], h4_send, h4_recv)

    zpad = jnp.zeros((NIM, 128), BF16)

    @pl.loop(0, ROWS + 2)
    def _(r):
        yy[0, r, pl.ds(0, NIM), :] = zpad
        yy[1, r, pl.ds(HALF * NIM, NIM), :] = zpad

    @pl.loop(0, OROWS + 2)
    def _(r):
        for c in (0, OCOLS + 1):
            y3[r, pl.ds(c * NIM, NIM), :] = jnp.zeros((NIM, 256), BF16)

    @pl.when(jnp.logical_not(has_far))
    def _():
        for b in range(2):
            yy[b, ROWS + 1] = jnp.zeros((YROW, 128), BF16)
        y3[OROWS + 1] = jnp.zeros((O3ROW, 256), BF16)

    def transpose_row(r):
        for n in range(NIM):
            tr[pl.ds(n * COLS, COLS), :] = xs[r, n].astype(F32)
        for j in range(COLS):
            v = tr[pl.ds(j, NIM, stride=COLS), :].astype(BF16)
            b, a = (j + 1) % 2, (j + 1) // 2
            yy[b, r, pl.ds(a * NIM, NIM), :] = v

    with jax.named_scope('transpose'):
        @pl.loop(0, 3)
        def _(r):
            x_copy(r).wait()
            transpose_row(r + 1)

    with jax.named_scope('barrier'):
        pl.semaphore_wait(barrier, GROUPS - 1)
    hx_near.start()

    @pl.when(has_far)
    def _():
        hx_far.start()

    for c in wa_copies:
        c.wait()
    zblk = jnp.zeros((128, 128), BF16)
    for layer in range(2):
        def put(k, lo, hi):
            wt[layer, pl.ds(k, 128), pl.ds(0, 128)] = zblk if lo is None else wraw[layer, lo[0], lo[1]]
            wt[layer, pl.ds(k, 128), pl.ds(128, 128)] = zblk if hi is None else wraw[layer, hi[0], hi[1]]
        for q in range(3):
            put(256 * q, (1, q), (0, q))
            put(256 * q + 128, (2, q), (1, q))
        for e, p in enumerate((0, 2)):
            k = 768 + 512 * e
            put(k, (p, 0), None)
            put(k + 128, (p, 1), (p, 0))
            put(k + 256, (p, 2), (p, 1))
            put(k + 384, None, (p, 2))

    with jax.named_scope('transpose2'):
        @pl.loop(3, 6)
        def _(r):
            x_copy(r).wait()
            transpose_row(r + 1)
    for c in w_copies:
        c.wait()

    def exchange(layer, rows):
        buf = jnp.concatenate(rows + [jnp.zeros((8 - len(rows), 128), F32)], axis=0)
        st_out[layer] = buf
        st_in[layer, me] = buf
        copies = []
        for k in range(1, GROUPS):
            copies.append(pltpu.make_async_remote_copy(
                src_ref=st_out.at[layer], dst_ref=st_in.at[layer, me],
                send_sem=st_send.at[layer, k], recv_sem=st_recv.at[layer, k],
                device_id=peer(k), device_id_type=MESH))
        for c in copies:
            c.start()
        with jax.named_scope(f'stat{layer}'):
            for c in copies:
                c.wait_recv()
        total = st_in[layer, 0]
        for s in range(1, GROUPS):
            total = total + st_in[layer, s]

        def finish():
            for c in copies:
                c.wait_send()
        return total, finish

    def moments(s1, s2, count):
        mean = s1 / count
        var = s2 / count - mean * mean
        return mean, lax.rsqrt(var + EPS_VALUE)

    def normalise(z, mean, inv, gamma, beta):
        return jnp.maximum(gamma * (z - mean) * inv + beta, 0.0).astype(BF16)

    TAPS = (((0, 0), (1, 0), (0, NIM)), ((1, 0), (0, NIM), (1, NIM)))
    QUAD = ((0, 0), (1, 0), (0, NIM), (1, NIM))

    def pair_layer(layer, ahead, before):
        def conv(i, carry):
            s1, s2 = carry
            for m in range(0, MROW, CHUNK):
                def take(taps, rows):
                    return jnp.concatenate(
                        [yy[plane, i + rr, pl.ds(m + off, CHUNK), :] for plane, off in taps for rr in rows], axis=1)
                mid = [jnp.dot(take(TAPS[b], (1, 2)), wt[layer, pl.ds(0, 768), :], preferred_element_type=F32)
                       for b in range(2)]
                edge = [jnp.dot(take(QUAD, (3 * e,)), wt[layer, pl.ds(768 + 512 * e, 512), :],
                                preferred_element_type=F32) for e in range(2)]
                for b in range(2):
                    for e in range(2):
                        z = mid[b][:, 128 * e:128 * e + 128] + edge[e][:, 128 * b:128 * b + 128]
                        zz[b, i + e, pl.ds(m, CHUNK), :] = z
                        z8 = z.reshape(CHUNK // 8, 8, 128)
                        s1 = s1 + jnp.sum(z8, axis=0)
                        s2 = s2 + jnp.sum(z8 * z8, axis=0)
            return s1, s2

        def first(it, carry):
            i = 2 * it
            if before is not None:
                before(it)
            ahead(i)
            return conv(i, carry)

        def second(it, carry):
            pair = jnp.where(it == 0, 4, (it - 1) * 5)

            @pl.when(it == 1)
            def _():
                with jax.named_scope(f'near{layer}'):
                    border_near(layer)

            @pl.when(it == 2)
            def _():
                with jax.named_scope(f'far{layer}'):
                    border_far(layer)
            return conv(2 * pair, carry)

        zero = jnp.zeros((8, 128), F32)
        with jax.named_scope(f'pairA{layer}'):
            carry = lax.fori_loop(1, 4, first, (zero, zero))
        with jax.named_scope(f'pairB{layer}'):
            s1, s2 = lax.fori_loop(0, 3, second, carry)
        total, finish = exchange(layer, [jnp.sum(s1, axis=0, keepdims=True), jnp.sum(s2, axis=0, keepdims=True)])
        mean, inv = moments(total[0:1], total[1:2], float(32 * 48 * 168))
        return mean, inv, finish

    def border_near(layer):
        if layer == 0:
            hx_near.wait_recv()
            transpose_row(0)
        else:
            h2_near.wait_recv()

    def border_far(layer):
        @pl.when(has_far)
        def _():
            if layer == 0:
                hx_far.wait_recv()
                transpose_row(ROWS + 1)
            else:
                h2_far.wait_recv()

    def norm_row(r, mean, inv, gamma, beta):
        yy[1, r + 1, pl.ds(0, MROW), :] = normalise(zz[0, r], mean, inv, gamma, beta)
        yy[0, r + 1, pl.ds(NIM, MROW), :] = normalise(zz[1, r], mean, inv, gamma, beta)

    def first_before(it):
        for e in range(2):
            x_copy(2 * it + 4 + e).wait()

    def first_ahead(i):
        transpose_row(i + 5)
        transpose_row(i + 6)

    mean, inv, fin1 = pair_layer(0, first_ahead, first_before)
    gamma, beta = nav[0, 0:1], nav[0, 1:2]

    with jax.named_scope('norm1'):
        norm_row(ROWS - 1, mean, inv, gamma, beta)

        @pl.when(has_far)
        def _():
            h2_far.start()
        norm_row(0, mean, inv, gamma, beta)
        h2_near.start()

        @pl.loop(1, 5)
        def _(r):
            norm_row(r, mean, inv, gamma, beta)

    def second_ahead(i):
        norm_row(i + 3, mean, inv, gamma, beta)
        norm_row(i + 4, mean, inv, gamma, beta)

    mean2, inv2, fin2 = pair_layer(1, second_ahead, None)
    gamma2, beta2 = nav[1, 0:1], nav[1, 1:2]
    h2_near.wait_send()

    @pl.when(has_far)
    def _():
        h2_far.wait_send()

    sends_near = flip == 0
    sends_far = sp == 2
    with jax.named_scope('norm2'):
        norm_row((ROWS - 1) * flip, mean2, inv2, gamma2, beta2)

        @pl.when(sends_near)
        def _():
            h3_near.start()

        @pl.when(sends_far)
        def _():
            h3_far.start()

        @pl.loop(1, ROWS)
        def _(r):
            norm_row(r - flip, mean2, inv2, gamma2, beta2)

    wd_taps = ((1, 0), (0, NIM), (1, NIM))

    def wide_conv(i, lhs_of, w_val, carry):
        s1, s2 = carry
        for m in range(0, OROW, CHUNK):
            lhs = jnp.concatenate(lhs_of(i, m), axis=1)
            res = jnp.dot(lhs, w_val, preferred_element_type=F32)
            z3[i, pl.ds(m, CHUNK), :] = res
            r3 = res.reshape(CHUNK // 8, 8, 256)
            s1 = s1 + jnp.sum(r3, axis=0)
            s2 = s2 + jnp.sum(r3 * r3, axis=0)
        return s1, s2

    def wide_stats(layer, carry):
        s1, s2 = carry
        s1 = jnp.sum(s1, axis=0, keepdims=True)
        s2 = jnp.sum(s2, axis=0, keepdims=True)
        total, finish = exchange(layer, [s1[:, :128], s1[:, 128:], s2[:, :128], s2[:, 128:]])
        s1 = jnp.concatenate([total[0:1], total[1:2]], axis=1)
        s2 = jnp.concatenate([total[2:3], total[3:4]], axis=1)
        mean, inv = moments(s1, s2, float(32 * 24 * 84))
        return mean, inv, finish

    zero = jnp.zeros((8, 256), F32)

    def down_lhs(i, m):
        return [yy[plane, 2 * i - flip + p + 1, pl.ds(m + off, CHUNK), :] for p in range(3) for plane, off in wd_taps]

    def down_body(it, carry):
        @pl.when(it == OROWS - 1)
        def _():
            with jax.named_scope('halo2'):
                @pl.when(flip == 1)
                def _():
                    h3_near.wait_recv()

                @pl.when(sp == 1)
                def _():
                    h3_far.wait_recv()
        return wide_conv(lax.rem(it + flip, OROWS), down_lhs, wdv[...].reshape(9 * 128, 256), carry)

    with jax.named_scope('wide2'):
        carry = lax.fori_loop(0, OROWS, down_body, (zero, zero))
    mean3, inv3, fin3 = wide_stats(2, carry)
    gamma3, beta3 = ndv[0:1], ndv[1:2]

    def norm3(r):
        y3[r + 1, pl.ds(NIM, OROW), :] = normalise(z3[r], mean3, inv3, gamma3, beta3)

    with jax.named_scope('norm3'):
        norm3(OROWS - 1)

        @pl.when(has_far)
        def _():
            h4_far.start()
        norm3(0)
        h4_near.start()

        @pl.loop(1, 3)
        def _(r):
            norm3(r)

    def last_lhs(i, m):
        return [y3[i + p, pl.ds(m + NIM * q, CHUNK), :] for p in range(3) for q in range(3)]

    wb_val = wbv[...].reshape(9 * 256, 256)

    def last_first(it, carry):
        norm3(it + 2)
        return wide_conv(it, last_lhs, wb_val, carry)

    def last_second(it, carry):
        i = jnp.where(it < 2, it + 3, (it - 2) * 5)

        @pl.when(it == 2)
        def _():
            with jax.named_scope('near3'):
                h4_near.wait_recv()

        @pl.when(it == 3)
        def _():
            with jax.named_scope('far3'):
                @pl.when(has_far)
                def _():
                    h4_far.wait_recv()
        return wide_conv(i, last_lhs, wb_val, carry)

    with jax.named_scope('wide3A'):
        carry = lax.fori_loop(1, 3, last_first, (zero, zero))
    with jax.named_scope('wide3B'):
        carry = lax.fori_loop(0, 4, last_second, carry)
    mean4, inv4, fin4 = wide_stats(3, carry)
    gamma4, beta4 = nbv[0, 0:1], nbv[0, 1:2]

    with jax.named_scope('out'):
        @pl.loop(0, OROWS)
        def _(r):
            out_ref[r + flip * (OROWS - 1 - 2 * r)] = normalise(z3[r], mean4, inv4, gamma4, beta4)

    with jax.named_scope('drain'):
        hx_near.wait_send()
        h4_near.wait_send()

        @pl.when(has_far)
        def _():
            hx_far.wait_send()
            h4_far.wait_send()

        @pl.when(sends_near)
        def _():
            h3_near.wait_send()

        @pl.when(sends_far)
        def _():
            h3_far.wait_send()
        for f in (fin1, fin2, fin3, fin4):
            f()


def solution(mesh):
    any_spec = pl.BlockSpec(memory_space=pl.ANY)
    dma = pltpu.SemaphoreType.DMA

    def local_stack(images, w_a, norm_a, w_down, norm_down, w_b, norm_b):
        out = pl.pallas_call(
            kernel,
            out_shape=pltpu.VMEM((OROWS, OROW, 256), BF16),
            in_specs=[any_spec] * 7,
            out_specs=pl.BlockSpec(memory_space=pltpu.VMEM),
            scratch_shapes=[
                pltpu.VMEM((ROWS + 2, NIM, COLS, 128), BF16),
                pltpu.VMEM((NIM * COLS, 128), F32),
                pltpu.VMEM((2, ROWS + 2, YROW, 128), BF16),
                pltpu.VMEM((2, ROWS, MROW, 128), F32),
                pltpu.VMEM((OROWS + 2, O3ROW, 256), BF16),
                pltpu.VMEM((OROWS, OROW, 256), F32),
                pltpu.VMEM((2, 3, 3, 128, 128), BF16),
                pltpu.VMEM((2, 1792, 256), BF16),
                pltpu.VMEM((3, 3, 128, 256), BF16),
                pltpu.VMEM((3, 3, 256, 256), BF16),
                pltpu.VMEM((2, 2, 128), F32),
                pltpu.VMEM((2, 256), F32),
                pltpu.VMEM((1, 2, 256), F32),
                pltpu.VMEM((4, 8, 128), F32),
                pltpu.VMEM((4, GROUPS, 8, 128), F32),
                dma((ROWS,)), dma((15,)),
                dma((2,)), dma((2,)), dma((2,)), dma((2,)), dma((2,)), dma((2,)), dma((2,)), dma((2,)),
                dma((4, GROUPS)), dma((4, GROUPS)),
            ],
            compiler_params=pltpu.CompilerParams(
                collective_id=0, has_side_effects=True, vmem_limit_bytes=VLIM),
        )(images, w_a, norm_a, w_down, norm_down, w_b.reshape(3, 3, 256, 256), norm_b)
        return jnp.transpose(out.reshape(OROWS, OCOLS, NIM, 256), (2, 0, 1, 3))

    act_spec = P(('pod', 'dp'), 'sp', None, None)
    return jax.shard_map(local_stack, mesh=mesh, in_specs=(act_spec, P(), P(), P(), P(), P(), P()), out_specs=act_spec, check_vma=False)
```

```python
import functools

import jax
import jax.numpy as jnp
from jax import lax
from jax.experimental import pallas as pl
from jax.experimental.pallas import tpu as pltpu
from jax.sharding import PartitionSpec as P

EPS_VALUE = 1e-5
F32 = jnp.float32
BF16 = jnp.bfloat16
MESH = pl.DeviceIdType.MESH

NIM = 16
ROWS = 12
COLS = 168
HALF = COLS // 2
MROW = HALF * NIM
YROW = (HALF + 1) * NIM
OROWS = 6
OCOLS = 84
OROW = OCOLS * NIM
O3ROW = (OCOLS + 2) * NIM
CHUNK = 336
NTR = 2
VLIM = 60 * 1024 * 1024
GROUPS = 8


def kernel(x_ref, wa_ref, na_ref, wd_ref, nd_ref, wb_ref, nb_ref, out_ref,
           xs, tr, yy, zz, y3, wraw, wt, wdv, wbv, nav, ndv, nbv,
           cf, st_out, st_in,
           x_sem, w_sem, hx_send, hx_recv, h2_send, h2_recv, h3_send, h3_recv, h4_send, h4_recv,
           st_send, st_recv):
    dp = lax.axis_index("dp")
    sp = lax.axis_index("sp")
    me = dp * 4 + sp
    flip = 1 - lax.rem(sp, 2)
    near = (0, dp, sp + 2 * flip - 1)
    far = (0, dp, lax.rem(7 - sp, 4))
    has_far = jnp.logical_or(sp == 1, sp == 2)

    def x_row(r):
        return r + flip * (ROWS - 1 - 2 * r)

    def tap(p):
        return p + flip * (2 - 2 * p)

    def x_copy(r):
        return pltpu.make_async_copy(x_ref.at[:, x_row(r)], xs.at[r + 1], x_sem.at[r])
    wa_copies = [pltpu.make_async_copy(wa_ref.at[l, tap(p)], wraw.at[l, p], w_sem.at[3 * l + p])
                 for l in range(2) for p in range(3)]
    w_copies = [pltpu.make_async_copy(na_ref, nav, w_sem.at[6]),
                pltpu.make_async_copy(nd_ref, ndv, w_sem.at[7]),
                pltpu.make_async_copy(nb_ref, nbv, w_sem.at[8])]
    for p in range(3):
        w_copies.append(pltpu.make_async_copy(wd_ref.at[tap(p)], wdv.at[p], w_sem.at[9 + p]))
        w_copies.append(pltpu.make_async_copy(wb_ref.at[tap(p)], wbv.at[p], w_sem.at[12 + p]))

    barrier = pltpu.get_barrier_semaphore()

    def peer(k):
        other = lax.rem(me + k, GROUPS)
        return (0, other // 4, lax.rem(other, 4))
    for k in range(1, GROUPS):
        pl.semaphore_signal(barrier, inc=1, device_id=peer(k), device_id_type=MESH)

    for r in range(3):
        x_copy(r).start()
    for c in wa_copies:
        c.start()
    for r in range(3, ROWS):
        x_copy(r).start()
    for c in w_copies:
        c.start()

    def halo(src_near, dst_near, src_far, dst_far, send, recv):
        n_copy = pltpu.make_async_remote_copy(
            src_ref=src_near, dst_ref=dst_near, send_sem=send.at[0], recv_sem=recv.at[0],
            device_id=near, device_id_type=MESH)
        f_copy = pltpu.make_async_remote_copy(
            src_ref=src_far, dst_ref=dst_far, send_sem=send.at[1], recv_sem=recv.at[1],
            device_id=far, device_id_type=MESH)
        return n_copy, f_copy

    hx_near, hx_far = halo(x_ref.at[:, x_row(0)], xs.at[0], x_ref.at[:, x_row(ROWS - 1)], xs.at[ROWS + 1],
                           hx_send, hx_recv)
    h2_near, h2_far = halo(yy.at[:, 1], yy.at[:, 0], yy.at[:, ROWS], yy.at[:, ROWS + 1], h2_send, h2_recv)
    h3_near, h3_far = halo(yy.at[:, 1], yy.at[:, 0], yy.at[:, ROWS], yy.at[:, ROWS + 1], h3_send, h3_recv)
    h4_near, h4_far = halo(y3.at[1], y3.at[0], y3.at[OROWS], y3.at[OROWS + 1], h4_send, h4_recv)

    zpad = jnp.zeros((NIM, 128), BF16)

    @pl.loop(0, ROWS + 2)
    def _(r):
        yy[0, r, pl.ds(0, NIM), :] = zpad
        yy[1, r, pl.ds(HALF * NIM, NIM), :] = zpad

    @pl.loop(0, OROWS + 2)
    def _(r):
        for c in (0, OCOLS + 1):
            y3[r, pl.ds(c * NIM, NIM), :] = jnp.zeros((NIM, 256), BF16)

    @pl.when(jnp.logical_not(has_far))
    def _():
        for b in range(2):
            yy[b, ROWS + 1] = jnp.zeros((YROW, 128), BF16)
        y3[OROWS + 1] = jnp.zeros((O3ROW, 256), BF16)

    def transpose_piece(r, lo, hi, slot):
        for n in range(NIM):
            tr[slot, pl.ds(n * COLS + lo, hi - lo), :] = xs[r, n, pl.ds(lo, hi - lo), :].astype(F32)
        for j in range(lo, hi):
            v = tr[slot, pl.ds(j, NIM, stride=COLS), :].astype(BF16)
            b, a = (j + 1) % 2, (j + 1) // 2
            yy[b, r, pl.ds(a * NIM, NIM), :] = v

    def transpose_row(r):
        transpose_piece(r, 0, COLS, 0)

    with jax.named_scope('transpose'):
        @pl.loop(0, 3)
        def _(r):
            x_copy(r).wait()
            transpose_row(r + 1)

    with jax.named_scope('barrier'):
        pl.semaphore_wait(barrier, GROUPS - 1)
    hx_near.start()

    @pl.when(has_far)
    def _():
        hx_far.start()

    for c in wa_copies:
        c.wait()
    zblk = jnp.zeros((128, 128), BF16)
    for layer in range(2):
        def put(k, lo, hi):
            wt[layer, pl.ds(k, 128), pl.ds(0, 128)] = zblk if lo is None else wraw[layer, lo[0], lo[1]]
            wt[layer, pl.ds(k, 128), pl.ds(128, 128)] = zblk if hi is None else wraw[layer, hi[0], hi[1]]
        for q in range(3):
            put(256 * q, (1, q), (0, q))
            put(256 * q + 128, (2, q), (1, q))
        for e, p in enumerate((0, 2)):
            k = 768 + 512 * e
            put(k, (p, 0), None)
            put(k + 128, (p, 1), (p, 0))
            put(k + 256, (p, 2), (p, 1))
            put(k + 384, None, (p, 2))

    with jax.named_scope('transpose2'):
        @pl.loop(3, 6)
        def _(r):
            x_copy(r).wait()
            transpose_row(r + 1)
    for c in w_copies:
        c.wait()

    def exchange(layer, rows):
        buf = jnp.concatenate(rows + [jnp.zeros((8 - len(rows), 128), F32)], axis=0)
        st_out[layer] = buf
        st_in[layer, me] = buf
        copies = []
        for k in range(1, GROUPS):
            copies.append(pltpu.make_async_remote_copy(
                src_ref=st_out.at[layer], dst_ref=st_in.at[layer, me],
                send_sem=st_send.at[layer, k], recv_sem=st_recv.at[layer, k],
                device_id=peer(k), device_id_type=MESH))
        for c in copies:
            c.start()
        with jax.named_scope(f'stat{layer}'):
            for c in copies:
                c.wait_recv()
        total = st_in[layer, 0]
        for s in range(1, GROUPS):
            total = total + st_in[layer, s]

        def finish():
            for c in copies:
                c.wait_send()
        return total, finish

    def moments(s1, s2, count):
        mean = s1 / count
        var = s2 / count - mean * mean
        return mean, lax.rsqrt(var + EPS_VALUE)

    def normalise(z, mean, inv, gamma, beta):
        return jnp.maximum(gamma * (z - mean) * inv + beta, 0.0).astype(BF16)

    TAPS = (((0, 0), (1, 0), (0, NIM)), ((1, 0), (0, NIM), (1, NIM)))
    QUAD = ((0, 0), (1, 0), (0, NIM), (1, NIM))

    def pair_layer(layer, ahead, before):
        def conv(i, carry, work=None):
            s1, s2 = carry
            for m in range(0, MROW, CHUNK):
                if work is not None:
                    work(i, m // CHUNK)
                def take(taps, rows):
                    return jnp.concatenate(
                        [yy[plane, i + rr, pl.ds(m + off, CHUNK), :] for plane, off in taps for rr in rows], axis=1)
                mid = [jnp.dot(take(TAPS[b], (1, 2)), wt[layer, pl.ds(0, 768), :], preferred_element_type=F32)
                       for b in range(2)]
                edge = [jnp.dot(take(QUAD, (3 * e,)), wt[layer, pl.ds(768 + 512 * e, 512), :],
                                preferred_element_type=F32) for e in range(2)]
                for b in range(2):
                    for e in range(2):
                        z = mid[b][:, 128 * e:128 * e + 128] + edge[e][:, 128 * b:128 * b + 128]
                        zz[b, i + e, pl.ds(m, CHUNK), :] = z
                        z8 = z.reshape(CHUNK // 8, 8, 128)
                        s1 = s1 + jnp.sum(z8, axis=0)
                        s2 = s2 + jnp.sum(z8 * z8, axis=0)
            return s1, s2

        def first(it, carry):
            i = 2 * it
            if before is not None:
                before(it)
            return conv(i, carry, ahead)


        zero = jnp.zeros((8, 128), F32)
        with jax.named_scope(f'pairA{layer}'):
            carry = (zero, zero)
            for it in range(1, 4):
                carry = first(it, carry)
            carry = conv(8, carry)
        with jax.named_scope(f'pairB{layer}'):
            with jax.named_scope(f'near{layer}'):
                border_near(layer)
            carry = conv(0, carry)
            with jax.named_scope(f'far{layer}'):
                border_far(layer)
            s1, s2 = conv(10, carry)
        total, finish = exchange(layer, [jnp.sum(s1, axis=0, keepdims=True), jnp.sum(s2, axis=0, keepdims=True)])
        mean, inv = moments(total[0:1], total[1:2], float(32 * 48 * 168))
        return mean, inv, finish

    def border_near(layer):
        if layer == 0:
            hx_near.wait_recv()
            transpose_row(0)
        else:
            h2_near.wait_recv()

    def border_far(layer):
        @pl.when(has_far)
        def _():
            if layer == 0:
                hx_far.wait_recv()
                transpose_row(ROWS + 1)
            else:
                h2_far.wait_recv()

    def norm_piece(r, m, size, coef):
        par = load_coef(coef)
        yy[1, r + 1, pl.ds(m, size), :] = normalise(zz[0, r, pl.ds(m, size), :], *par)
        yy[0, r + 1, pl.ds(NIM + m, size), :] = normalise(zz[1, r, pl.ds(m, size), :], *par)

    def norm_row(r, coef):
        norm_piece(r, 0, MROW, coef)

    def save_coef(slot, width, mean, inv, gamma, beta):
        for k, v in enumerate((mean, inv, gamma, beta)):
            cf[slot, k:k + 1, pl.ds(0, width)] = v
        return slot

    def load_coef(slot, lane=0):
        return [cf[slot, k:k + 1, pl.ds(lane, 128)] for k in range(4)]

    def first_before(it):
        if it == 1:
            for r in range(6, ROWS):
                x_copy(r).wait()

    def first_ahead(i, c):
        for e in range(2):
            transpose_piece(i + 5 + e, 48 * c, min(48 * c + 48, COLS), e % NTR)

    mean, inv, fin1 = pair_layer(0, first_ahead, first_before)
    coef1 = save_coef(0, 128, mean, inv, nav[0, 0:1], nav[0, 1:2])

    with jax.named_scope('norm1'):
        norm_row(ROWS - 1, coef1)

        @pl.when(has_far)
        def _():
            h2_far.start()
        norm_row(0, coef1)
        h2_near.start()

        @pl.loop(1, 5)
        def _(r):
            norm_row(r, coef1)

    def second_ahead(i, c):
        for e in range(2):
            norm_piece(i + 3 + e, c * CHUNK, CHUNK, coef1)

    mean2, inv2, fin2 = pair_layer(1, second_ahead, None)
    coef2 = save_coef(1, 128, mean2, inv2, nav[1, 0:1], nav[1, 1:2])
    h2_near.wait_send()

    @pl.when(has_far)
    def _():
        h2_far.wait_send()

    sends_near = flip == 0
    sends_far = sp == 2
    with jax.named_scope('norm2'):
        norm_row((ROWS - 1) * flip, coef2)

        @pl.when(sends_near)
        def _():
            h3_near.start()

        @pl.when(sends_far)
        def _():
            h3_far.start()

        @pl.loop(1, ROWS)
        def _(r):
            norm_row(r - flip, coef2)

    wd_taps = ((1, 0), (0, NIM), (1, NIM))

    def wide_conv(i, lhs_of, w_val, carry, work=None):
        s1, s2 = carry
        for m in range(0, OROW, CHUNK):
            if work is not None:
                work(m)
            lhs = jnp.concatenate(lhs_of(i, m), axis=1)
            res = jnp.dot(lhs, w_val, preferred_element_type=F32)
            zz[0, i, pl.ds(m, CHUNK), :] = res[:, :128]
            zz[1, i, pl.ds(m, CHUNK), :] = res[:, 128:]
            r3 = res.reshape(CHUNK // 8, 8, 256)
            s1 = s1 + jnp.sum(r3, axis=0)
            s2 = s2 + jnp.sum(r3 * r3, axis=0)
        return s1, s2

    def wide_stats(layer, carry):
        s1, s2 = carry
        s1 = jnp.sum(s1, axis=0, keepdims=True)
        s2 = jnp.sum(s2, axis=0, keepdims=True)
        total, finish = exchange(layer, [s1[:, :128], s1[:, 128:], s2[:, :128], s2[:, 128:]])
        s1 = jnp.concatenate([total[0:1], total[1:2]], axis=1)
        s2 = jnp.concatenate([total[2:3], total[3:4]], axis=1)
        mean, inv = moments(s1, s2, float(32 * 24 * 84))
        return mean, inv, finish

    zero = jnp.zeros((8, 256), F32)

    def down_lhs(i, m):
        return [yy[plane, 2 * i - flip + p + 1, pl.ds(m + off, CHUNK), :] for p in range(3) for plane, off in wd_taps]

    wd_val = wdv[...].reshape(9 * 128, 256)
    with jax.named_scope('wide2'):
        carry = (zero, zero)
        for it in range(OROWS - 1):
            carry = wide_conv(it + flip, down_lhs, wd_val, carry)
    with jax.named_scope('halo2'):
        @pl.when(flip == 1)
        def _():
            h3_near.wait_recv()

        @pl.when(sp == 1)
        def _():
            h3_far.wait_recv()
    with jax.named_scope('wide2B'):
        carry = wide_conv((OROWS - 1) * (1 - flip), down_lhs, wd_val, carry)
    mean3, inv3, fin3 = wide_stats(2, carry)
    coef3 = save_coef(2, 256, mean3, inv3, ndv[0:1], ndv[1:2])

    def norm3_piece(r, m, size):
        for h in range(2):
            par = load_coef(coef3, 128 * h)
            y3[r + 1, pl.ds(NIM + m, size), pl.ds(128 * h, 128)] = normalise(zz[h, r, pl.ds(m, size), :], *par)

    def norm3(r):
        norm3_piece(r, 0, OROW)

    with jax.named_scope('norm3'):
        norm3(OROWS - 1)

        @pl.when(has_far)
        def _():
            h4_far.start()
        norm3(0)
        h4_near.start()

        @pl.loop(1, 3)
        def _(r):
            norm3(r)

    def last_lhs(i, m):
        return [y3[i + p, pl.ds(m + NIM * q, CHUNK), :] for p in range(3) for q in range(3)]

    wb_val = wbv[...].reshape(9 * 256, 256)

    def last_first(it, carry):
        return wide_conv(it, last_lhs, wb_val, carry, lambda m: norm3_piece(it + 2, m, CHUNK))


    with jax.named_scope('wide3A'):
        carry = (zero, zero)
        for it in range(1, 3):
            carry = last_first(it, carry)
    with jax.named_scope('wide3B'):
        for it in (3, 4):
            carry = wide_conv(it, last_lhs, wb_val, carry)
        with jax.named_scope('near3'):
            h4_near.wait_recv()
        carry = wide_conv(0, last_lhs, wb_val, carry)
        with jax.named_scope('far3'):
            @pl.when(has_far)
            def _():
                h4_far.wait_recv()
        carry = wide_conv(OROWS - 1, last_lhs, wb_val, carry)
    mean4, inv4, fin4 = wide_stats(3, carry)
    coef4 = save_coef(3, 256, mean4, inv4, nbv[0, 0:1], nbv[0, 1:2])

    with jax.named_scope('out'):
        @pl.loop(0, OROWS)
        def _(r):
            for h in range(2):
                out_ref[r + flip * (OROWS - 1 - 2 * r), :, pl.ds(128 * h, 128)] = normalise(
                    zz[h, r], *load_coef(coef4, 128 * h))

    with jax.named_scope('drain'):
        hx_near.wait_send()
        h4_near.wait_send()

        @pl.when(has_far)
        def _():
            hx_far.wait_send()
            h4_far.wait_send()

        @pl.when(sends_near)
        def _():
            h3_near.wait_send()

        @pl.when(sends_far)
        def _():
            h3_far.wait_send()
        for f in (fin1, fin2, fin3, fin4):
            f()


def solution(mesh):
    any_spec = pl.BlockSpec(memory_space=pl.ANY)
    dma = pltpu.SemaphoreType.DMA

    def local_stack(images, w_a, norm_a, w_down, norm_down, w_b, norm_b):
        out = pl.pallas_call(
            kernel,
            out_shape=pltpu.VMEM((OROWS, OROW, 256), BF16),
            in_specs=[any_spec] * 7,
            out_specs=pl.BlockSpec(memory_space=pltpu.VMEM),
            scratch_shapes=[
                pltpu.VMEM((ROWS + 2, NIM, COLS, 128), BF16),
                pltpu.VMEM((NTR, NIM * COLS, 128), F32),
                pltpu.VMEM((2, ROWS + 2, YROW, 128), BF16),
                pltpu.VMEM((2, ROWS, MROW, 128), F32),
                pltpu.VMEM((OROWS + 2, O3ROW, 256), BF16),
                pltpu.VMEM((2, 3, 3, 128, 128), BF16),
                pltpu.VMEM((2, 1792, 256), BF16),
                pltpu.VMEM((3, 3, 128, 256), BF16),
                pltpu.VMEM((3, 3, 256, 256), BF16),
                pltpu.VMEM((2, 2, 128), F32),
                pltpu.VMEM((2, 256), F32),
                pltpu.VMEM((1, 2, 256), F32),
                pltpu.VMEM((4, 8, 256), F32),
                pltpu.VMEM((4, 8, 128), F32),
                pltpu.VMEM((4, GROUPS, 8, 128), F32),
                dma((ROWS,)), dma((15,)),
                dma((2,)), dma((2,)), dma((2,)), dma((2,)), dma((2,)), dma((2,)), dma((2,)), dma((2,)),
                dma((4, GROUPS)), dma((4, GROUPS)),
            ],
            compiler_params=pltpu.CompilerParams(
                collective_id=0, has_side_effects=True, vmem_limit_bytes=VLIM),
        )(images, w_a, norm_a, w_down, norm_down, w_b.reshape(3, 3, 256, 256), norm_b)
        return jnp.transpose(out.reshape(OROWS, OCOLS, NIM, 256), (2, 0, 1, 3))

    act_spec = P(('pod', 'dp'), 'sp', None, None)
    return jax.shard_map(local_stack, mesh=mesh, in_specs=(act_spec, P(), P(), P(), P(), P(), P()), out_specs=act_spec, check_vma=False)
```

```python
import functools

import jax
import jax.numpy as jnp
from jax import lax
from jax.experimental import pallas as pl
from jax.experimental.pallas import tpu as pltpu
from jax.sharding import PartitionSpec as P

EPS_VALUE = 1e-5
F32 = jnp.float32
BF16 = jnp.bfloat16
MESH = pl.DeviceIdType.MESH

NIM = 16
ROWS = 12
COLS = 168
HALF = COLS // 2
MROW = HALF * NIM
YROW = (HALF + 1) * NIM
OROWS = 6
OCOLS = 84
OROW = OCOLS * NIM
O3ROW = (OCOLS + 2) * NIM
CHUNK = 336
NTR = 2
VLIM = 56 * 1024 * 1024
GROUPS = 8
LANES = 128
WIDE = 256
LAST, FAR_SLOT = ROWS - 1, ROWS + 1
OLAST, OFAR = OROWS - 1, OROWS + 1
TWO_CHUNKS = 2 * CHUNK
SUB = CHUNK // 8
PIECES = range(0, MROW, CHUNK)


def head(size):
    return pl.ds(0, size)


def join(parts):
    return jnp.concatenate(parts, axis=1)


def mm(lhs, rhs):
    return jnp.dot(lhs, rhs, preferred_element_type=F32)


def sublane_sum(val):
    return jnp.sum(val, axis=0)


def column_sum(val):
    return jnp.sum(val, axis=0, keepdims=True)


def kernel(x_ref, wa_ref, na_ref, wd_ref, nd_ref, wb_ref, nb_ref, z_out, c_out,
           xs, tr, yy, zz, zo, y3, yx, ys, wx, wt, wdv, wbv, nav, ndv, nbv,
           cf, st_out, st_in, sw_out, sw_in,
           x_sem, w_sem, hx_send, hx_recv, h2_send, h2_recv, h3_send, h3_recv, h4_send, h4_recv,
           st_send, st_recv):
    dp = lax.axis_index("dp")
    sp = lax.axis_index("sp")
    me = dp * 4 + sp
    upright = lax.rem(sp, 2)
    flip = 1 - upright
    near = (0, dp, sp + 2 * flip - 1)
    far = (0, dp, lax.rem(7 - sp, 4))
    has_far = jnp.logical_or(sp == 1, sp == 2)

    def x_row(r):
        return r + flip * (LAST - 2 * r)

    def tap(p):
        return p + flip * (2 - 2 * p)

    def x_slot(r):
        return {9: 1, 10: 2, 11: 10, 0: 11}.get(r, r)

    def x_copy(r):
        return pltpu.make_async_copy(x_ref.at[:, x_row(r)], xs.at[x_slot(r)], x_sem.at[r])
    wa_copies = [pltpu.make_async_copy(wa_ref.at[l, tap(p)], ys.at[l, pl.ds(384 * p, 384)], w_sem.at[3 * l + p])
                 for l in range(2) for p in range(3)]
    w_copies = [pltpu.make_async_copy(na_ref, nav, w_sem.at[6]),
                pltpu.make_async_copy(nd_ref, ndv, w_sem.at[7]),
                pltpu.make_async_copy(nb_ref, nbv, w_sem.at[8])]
    for p in range(3):
        w_copies.append(pltpu.make_async_copy(wd_ref.at[tap(p)], wdv.at[p], w_sem.at[9 + p]))
        w_copies.append(pltpu.make_async_copy(wb_ref.at[tap(p)], wbv.at[p], w_sem.at[12 + p]))

    barrier = pltpu.get_barrier_semaphore()

    def peer(k):
        x, core = sp // 2, lax.rem(sp, 2)
        x = 1 - x if k & 2 else x
        core = 1 - core if k & 1 else core
        return (0, 1 - dp if k & 4 else dp, 2 * x + core)
    for k in range(1, GROUPS):
        pl.semaphore_signal(barrier, inc=1, device_id=peer(k), device_id_type=MESH)

    for r in (1, 2):
        x_copy(r).start()
    for c in wa_copies:
        c.start()
    for r in (3, 4, 5, 6, 7, 8, 11, 0):
        x_copy(r).start()
    for c in w_copies:
        c.start()

    def halo(src_near, dst_near, src_far, dst_far, send, recv):
        n_copy = pltpu.make_async_remote_copy(
            src_ref=src_near, dst_ref=dst_near, send_sem=send.at[0], recv_sem=recv.at[0],
            device_id=near, device_id_type=MESH)
        f_copy = pltpu.make_async_remote_copy(
            src_ref=src_far, dst_ref=dst_far, send_sem=send.at[1], recv_sem=recv.at[1],
            device_id=far, device_id_type=MESH)
        return n_copy, f_copy

    hx_near, hx_far = halo(x_ref.at[:, x_row(0)], xs.at[0], x_ref.at[:, x_row(LAST)], xs.at[9],
                           hx_send, hx_recv)
    h2_near, h2_far = halo(yy.at[:, 1], yy.at[:, 0], yy.at[:, ROWS], yy.at[:, FAR_SLOT], h2_send, h2_recv)
    h3_near, hy0 = halo(yy.at[:, 1], yy.at[:, FAR_SLOT], ys.at[0], yx.at[0], h3_send, h3_recv)
    hy1 = pltpu.make_async_remote_copy(
        src_ref=ys.at[1], dst_ref=yx.at[1], send_sem=h3_send.at[2], recv_sem=h3_recv.at[2],
        device_id=far, device_id_type=MESH)
    h4_near, h4_far = halo(y3.at[1], y3.at[0], y3.at[OROWS], y3.at[OFAR], h4_send, h4_recv)

    zpad = jnp.zeros((NIM, LANES), BF16)

    @pl.loop(0, ROWS + 2)
    def _(r):
        yy[0, r, head(NIM), :] = zpad
        yy[1, r, pl.ds(HALF * NIM, NIM), :] = zpad


    @pl.loop(0, OROWS + 2)
    def _(r):
        for c in (0, OCOLS + 1):
            y3[r, pl.ds(c * NIM, NIM), :] = jnp.zeros((NIM, WIDE), BF16)

    @pl.when(jnp.logical_not(has_far))
    def _():
        for b in range(2):
            yy[b, FAR_SLOT] = jnp.zeros((YROW, LANES), BF16)
        y3[OFAR] = jnp.zeros((O3ROW, WIDE), BF16)

    def transpose_piece(r, lo, hi, slot, src):
        for n in range(NIM):
            tr[slot, pl.ds(n * COLS + lo, hi - lo), :] = xs[src, n, pl.ds(lo, hi - lo), :].astype(F32)
        for j in range(lo, hi):
            v = tr[slot, pl.ds(j, NIM, stride=COLS), :].astype(BF16)
            b, a = (j + 1) % 2, (j + 1) // 2
            yy[b, r, pl.ds(a * NIM, NIM), :] = v

    def transpose_row(r, src):
        transpose_piece(r, 0, COLS, 0, src)

    with jax.named_scope('transpose'):
        @pl.loop(1, 3)
        def _(r):
            pltpu.make_async_copy(x_ref.at[:, x_row(r)], xs.at[r], x_sem.at[r]).wait()
            transpose_row(r + 1, r)
    for r in (9, 10):
        x_copy(r).start()

    with jax.named_scope('barrier'):
        pl.semaphore_wait(barrier, GROUPS - 1)

    @pl.when(has_far)
    def _():
        hx_far.start()
    hx_near.start()

    for c in wa_copies:
        c.wait()
    zblk = jnp.zeros((LANES, LANES), BF16)

    def tile(layer, p, q):
        return zblk if q is None else ys[layer, pl.ds(384 * p + LANES * q, LANES), :]

    for layer in range(2):
        def put(k, lo, hi):
            wt[layer, pl.ds(k, LANES), head(LANES)] = tile(layer, *lo)
            wt[layer, pl.ds(k, LANES), pl.ds(LANES, LANES)] = tile(layer, *hi)
        for q in range(3):
            put(WIDE * q, (1, q), (0, q))
            put(WIDE * q + LANES, (2, q), (1, q))
        for e, p in enumerate((0, 2)):
            k = 768 + 512 * e
            put(k, (p, 0), (p, None))
            put(k + LANES, (p, 1), (p, 0))
            put(k + WIDE, (p, 2), (p, 1))
            put(k + 384, (p, None), (p, 2))
    for k, (lo, hi) in enumerate(((0, None), (1, 0), (2, 1), (None, 2))):
        wx[pl.ds(LANES * k, LANES), head(LANES)] = tile(1, 1, lo)
        wx[pl.ds(LANES * k, LANES), pl.ds(LANES, LANES)] = tile(1, 1, hi)

    ys[0, head(NIM), :] = zpad
    ys[1, pl.ds(HALF * NIM, NIM), :] = zpad

    with jax.named_scope('transpose2'):
        @pl.loop(3, 5)
        def _(r):
            pltpu.make_async_copy(x_ref.at[:, x_row(r)], xs.at[r], x_sem.at[r]).wait()
            transpose_row(r + 1, r)
    for r in (5, 6, 7, 8, 11, 0, 9, 10):
        x_copy(r).wait()
    for c in w_copies:
        c.wait()

    def exchange(layer, rows, meanwhile=None):
        out, slots = (st_out, st_in) if layer < 2 else (sw_out, sw_in)
        at = layer % 2
        buf = join(rows)
        out[at] = buf
        slots[at, me] = buf
        copies = []
        for k in (7, 6, 5, 4, 3, 2, 1):
            copies.append(pltpu.make_async_remote_copy(
                src_ref=out.at[at], dst_ref=slots.at[at, me],
                send_sem=st_send.at[layer, k], recv_sem=st_recv.at[layer, k],
                device_id=peer(k), device_id_type=MESH))
        for c in copies:
            c.start()
        if meanwhile is not None:
            meanwhile()
        with jax.named_scope(f'stat{layer}'):
            for c in copies:
                c.wait_recv()
        total = slots[at, 0]
        for s in range(1, GROUPS):
            total = total + slots[at, s]

        def finish():
            for c in copies:
                c.wait_send()
        half = total.shape[1] // 2
        return total[:, :half], total[:, half:], finish

    def moments(s1, s2, count):
        mean = s1 / count
        var = s2 / count - mean * mean
        return mean, lax.rsqrt(var + EPS_VALUE)

    def normalise(z, mean, inv, gamma, beta):
        return jnp.maximum(gamma * (z - mean) * inv + beta, 0.0).astype(BF16)

    TAPS = (((0, 0), (1, 0), (0, NIM)), ((1, 0), (0, NIM), (1, NIM)))
    QUAD = ((0, 0), (1, 0), (0, NIM), (1, NIM))

    def pair_layer(layer, ahead, near_row, far_row, meanwhile=None):
        def conv(i, carry, work=None):
            s1, s2 = carry
            for m in PIECES:
                if work is not None:
                    work(i, m // CHUNK)
                def take(taps, rows):
                    return join(
                        [yy[plane, i + rr, pl.ds(m + off, CHUNK), :] for plane, off in taps for rr in rows])
                mid = [mm(take(TAPS[b], (1, 2)), wt[layer, head(768), :])
                       for b in range(2)]
                edge = [mm(take(QUAD, (3 * e,)), wt[layer, pl.ds(768 + 512 * e, 512), :]) for e in range(2)]
                for b in range(2):
                    for e in range(2):
                        z = mid[b][:, LANES * e:LANES * e + LANES] + edge[e][:, LANES * b:LANES * b + LANES]
                        zz[b, i + e, pl.ds(m, CHUNK), :] = z
                        z8 = z.reshape(SUB, 8, LANES)
                        s1 = s1 + sublane_sum(z8)
                        s2 = s2 + sublane_sum(z8 * z8)
            return s1, s2

        def border(it, carry):
            @pl.when(it == 0)
            def _():
                near_row.wait_recv()

            @pl.when(jnp.logical_and(it == 1, has_far))
            def _():
                far_row.wait_recv()
            if layer == 0:
                @pl.when(jnp.logical_or(it == 0, has_far))
                def _():
                    transpose_row(it * (FAR_SLOT), it * 9)
            return conv(10 * it, carry)

        zero = jnp.zeros((8, LANES), F32)
        carry = (zero, zero)
        with jax.named_scope(f'pairA{layer}'):
            for i in (2, 4, 6, 8):
                carry = conv(i, carry, ahead)
        if layer == 1:
            @pl.when(sp == 2)
            def _():
                hy0.start()
        with jax.named_scope(f'pairB{layer}'):
            s1, s2 = lax.fori_loop(0, 2, border, carry)
        s1, s2, finish = exchange(layer, [column_sum(s1), column_sum(s2)],
                                  meanwhile)
        mean, inv = moments(s1, s2, float(32 * 48 * 168))
        return mean, inv, finish

    def norm_piece(r, m, size, coef, slot=None, copy_too=False):
        par = load_coef(coef)
        slot = r + 1 if slot is None else slot
        for b, plane, off in ((0, 1, m), (1, 0, NIM + m)):
            val = normalise(zz[b, r, pl.ds(m, size), :], *par)
            yy[plane, slot, pl.ds(off, size), :] = val
            if copy_too:
                ys[plane, pl.ds(off, size), :] = val

    def norm_row(r, coef):
        norm_piece(r, 0, MROW, coef)

    def save_coef(slot, width, mean, inv, gamma, beta):
        for k, v in enumerate((mean, inv, gamma, beta)):
            cf[slot, k:k + 1, head(width)] = v
        return slot

    def load_coef(slot, lane=0):
        return [cf[slot, k:k + 1, pl.ds(lane, LANES)] for k in range(4)]

    def first_ahead(i, c):
        for e in range(2):
            r = i + 3 + e if i < 8 else (LAST) * (1 - e)
            transpose_piece(r + 1, 48 * c, min(48 * c + 48, COLS), e % NTR, x_slot(r))

    mean, inv, fin1 = pair_layer(0, first_ahead, hx_near, hx_far)
    coef1 = save_coef(0, LANES, mean, inv, nav[0, 0:1], nav[0, 1:2])

    with jax.named_scope('norm1'):
        norm_row(LAST, coef1)

        @pl.when(has_far)
        def _():
            h2_far.start()
        norm_row(0, coef1)
        h2_near.start()

        @pl.loop(1, 5)
        def _(r):
            norm_piece(r, 0, TWO_CHUNKS, coef1)

    def second_ahead(i, c):
        if i == 2 and c < 2:
            for r in range(1, 5):
                norm_piece(r, (c + 2) * CHUNK, CHUNK, coef1)
        if i < 8:
            for r in (i + 3, i + 4):
                if r < LAST:
                    norm_piece(r, c * CHUNK, CHUNK, coef1, None, r == ROWS - 2)

    def lone_row(m, taps):
        res = None
        for p in taps:
            src = (yy.at[:, ROWS], yy.at[:, FAR_SLOT], yx)[p]
            lhs = join([src[plane, pl.ds(m + off, CHUNK), :] for plane, off in QUAD])
            w_val = wx[...] if p == 1 else wt[1, pl.ds(768 + WIDE * p, 512), :]
            part = mm(lhs, w_val)
            res = part if res is None else res + part
        return res

    def second_meanwhile():
        @pl.when(sp == 2)
        def _():
            hy1.start()

        @pl.when(sp == 1)
        def _():
            for m in PIECES:
                res = lone_row(m, (0, 1))
                tr[0, pl.ds(m, CHUNK), :] = res[:, :LANES]
                tr[1, pl.ds(m, CHUNK), :] = res[:, LANES:]

    mean2, inv2, fin2 = pair_layer(1, second_ahead, h2_near, h2_far, second_meanwhile)
    coef2 = save_coef(1, LANES, mean2, inv2, nav[1, 0:1], nav[1, 1:2])
    h2_near.wait_send()

    @pl.when(has_far)
    def _():
        h2_far.wait_send()

    sends_near = upright == 1
    with jax.named_scope('norm2'):
        norm_piece(flip, 0, MROW, coef2, 1)

        @pl.when(sends_near)
        def _():
            h3_near.start()
        for r in (1, 2):
            norm_piece(r + flip, 0, TWO_CHUNKS, coef2, r + 1)

    wd_taps = ((1, 0), (0, NIM), (1, NIM))

    def wide_conv(dst, i, lhs_of, w_val, carry, work=None):
        s1, s2 = carry
        for m in PIECES:
            if work is not None:
                work(m)
            lhs = join(lhs_of(m))
            res = mm(lhs, w_val)
            dst[0, i, pl.ds(m, CHUNK), :] = res[:, :LANES]
            dst[1, i, pl.ds(m, CHUNK), :] = res[:, LANES:]
            r3 = res.reshape(SUB, 8, WIDE)
            s1 = s1 + sublane_sum(r3)
            s2 = s2 + sublane_sum(r3 * r3)
        return s1, s2

    def wide_stats(layer, carry):
        s1, s2 = carry
        s1, s2, finish = exchange(layer, [column_sum(s1), column_sum(s2)])
        mean, inv = moments(s1, s2, float(32 * 24 * 84))
        return mean, inv, finish

    zero = jnp.zeros((8, WIDE), F32)

    def down_lhs(slots):
        return lambda m: [yy[plane, slot, pl.ds(m + off, CHUNK), :] for slot in slots for plane, off in wd_taps]

    wd_val = wdv[...].reshape(9 * LANES, WIDE)

    def down_ahead(it):
        def work(m):
            if it == 0 and m < TWO_CHUNKS:
                for r in (1, 2):
                    norm_piece(r + flip, m + TWO_CHUNKS, CHUNK, coef2, r + 1)
            for e in range(2):
                norm_piece(2 * it + 3 + e + flip, m, CHUNK, coef2, 2 * it + 4 + e)
        return work if it < 4 else None

    with jax.named_scope('wide2'):
        carry = (zero, zero)
        for it in range(OLAST):
            carry = wide_conv(zo, it, down_lhs((2 * it + 1, 2 * it + 2, 2 * it + 3)), wd_val, carry, down_ahead(it))

    with jax.named_scope('halo2'):
        @pl.when(sp == 1)
        def _():
            hy0.wait_recv()
            hy1.wait_recv()

            par = load_coef(coef2)
            for m in PIECES:
                res = lone_row(m, (2,))
                for b, plane, off in ((0, 1, m), (1, 0, NIM + m)):
                    z = tr[b, pl.ds(m, CHUNK), :] + res[:, LANES * b:LANES * b + LANES]
                    yy[plane, FAR_SLOT, pl.ds(off, CHUNK), :] = normalise(z, *par)

        norm_piece((LAST) * upright, 0, MROW, coef2, ROWS * upright)

        @pl.when(flip == 1)
        def _():
            h3_near.wait_recv()
    with jax.named_scope('wide2B'):
        slots = (LAST + 2 * flip, ROWS * upright, FAR_SLOT - ROWS * flip)
        carry = wide_conv(zo, OLAST, down_lhs(slots), wd_val, carry)
    mean3, inv3, fin3 = wide_stats(2, carry)
    coef3 = save_coef(2, WIDE, mean3, inv3, ndv[0:1], ndv[1:2])

    def norm3_piece(r, m, size):
        step = lax.rem(r - flip + OROWS, OROWS)
        for h in range(2):
            par = load_coef(coef3, LANES * h)
            y3[r + 1, pl.ds(NIM + m, size), pl.ds(LANES * h, LANES)] = normalise(zo[h, step, pl.ds(m, size), :], *par)

    def norm3(r):
        norm3_piece(r, 0, OROW)

    with jax.named_scope('norm3'):
        norm3(OLAST)

        @pl.when(has_far)
        def _():
            h4_far.start()

        norm3(0)
        h4_near.start()

        @pl.loop(1, 3)
        def _(r):
            norm3_piece(r, 0, TWO_CHUNKS)

    def last_lhs(i, taps=(0, 1, 2)):
        return lambda m: [y3[i + p, pl.ds(m + NIM * q, CHUNK), :] for p in taps for q in range(3)]

    wb_val = wbv[...].reshape(9 * WIDE, WIDE)

    def last_ahead(it):
        def work(m):
            if it == 1:
                if m < TWO_CHUNKS:
                    for r in range(1, 3):
                        norm3_piece(r, m + TWO_CHUNKS, CHUNK)
                norm3_piece(3, m, CHUNK)
            elif it == 2:
                norm3_piece(4, m, CHUNK)
        return work

    with jax.named_scope('wide3A'):
        carry = (zero, zero)
        for it in (1, 2, 3, 4):
            carry = wide_conv(z_out, it, last_lhs(it), wb_val, carry, last_ahead(it))
    with jax.named_scope('wide3B'):
        with jax.named_scope('near3'):
            h4_near.wait_recv()
        carry = wide_conv(z_out, 0, last_lhs(0), wb_val, carry)
        part_w = wbv[head(2)].reshape(6 * WIDE, WIDE)
        last_w = wbv[2].reshape(3 * WIDE, WIDE)
        r = OLAST
        for m in PIECES:
            res = mm(join(last_lhs(r, (0, 1))(m)), part_w)
            z_out[0, r, pl.ds(m, CHUNK), :] = res[:, :LANES]
            z_out[1, r, pl.ds(m, CHUNK), :] = res[:, LANES:]
        with jax.named_scope('far3'):
            @pl.when(has_far)
            def _():
                h4_far.wait_recv()
        s1, s2 = carry
        for m in PIECES:
            res = mm(join(last_lhs(r, (2,))(m)), last_w)
            res = res + join([z_out[h, r, pl.ds(m, CHUNK), :] for h in range(2)])
            z_out[0, r, pl.ds(m, CHUNK), :] = res[:, :LANES]
            z_out[1, r, pl.ds(m, CHUNK), :] = res[:, LANES:]
            r3 = res.reshape(SUB, 8, WIDE)
            s1 = s1 + sublane_sum(r3)
            s2 = s2 + sublane_sum(r3 * r3)
        carry = s1, s2
    mean4, inv4, fin4 = wide_stats(3, carry)
    for k, v in enumerate((mean4, inv4, nbv[0, 0:1], nbv[0, 1:2])):
        c_out[k:k + 1] = v

    with jax.named_scope('drain'):
        hx_near.wait_send()
        h4_near.wait_send()

        @pl.when(has_far)
        def _():
            hx_far.wait_send()
            h4_far.wait_send()

        @pl.when(sends_near)
        def _():
            h3_near.wait_send()

        @pl.when(sp == 2)
        def _():
            hy0.wait_send()
            hy1.wait_send()
        for f in (fin1, fin2, fin3, fin4):
            f()


def result_kernel(z_ref, c_ref, out_ref, yo, cf, sem):
    flip = 1 - lax.rem(lax.axis_index("sp"), 2)

    def copy(r):
        return pltpu.make_async_copy(yo.at[r], out_ref.at[r + flip * (OLAST - 2 * r)], sem.at[r])

    mean, inv, gamma, beta = [c_ref[k:k + 1] for k in range(4)]
    scale = gamma * inv
    cf[0:1] = scale
    cf[1:2] = beta - mean * scale
    small = jnp.logical_and(jnp.max(jnp.abs(scale)) < 1e15, jnp.max(jnp.abs(mean)) < 1e20)

    @pl.when(small)
    def _():
        @pl.loop(0, OROWS)
        def _(r):
            for h in range(2):
                lanes = pl.ds(LANES * h, LANES)
                y = z_ref[h, r] * cf[0:1, lanes] + cf[1:2, lanes]
                yo[r, :, lanes] = jnp.maximum(y, 0.0).astype(BF16)
            copy(r).start()

    @pl.when(jnp.logical_not(small))
    def _():
        @pl.loop(0, OROWS)
        def _(r):
            for h in range(2):
                lanes = pl.ds(LANES * h, LANES)
                mean, inv, gamma, beta = [c_ref[k:k + 1, lanes] for k in range(4)]
                yo[r, :, lanes] = jnp.maximum(gamma * (z_ref[h, r] - mean) * inv + beta, 0.0).astype(BF16)
            copy(r).start()

    @pl.loop(0, OROWS)
    def _(r):
        copy(r).wait()


def solution(mesh):
    any_spec = pl.BlockSpec(memory_space=pl.ANY)
    dma = pltpu.SemaphoreType.DMA

    def local_stack(images, w_a, norm_a, w_down, norm_down, w_b, norm_b):
        z_last, coef = pl.pallas_call(
            kernel,
            out_shape=(pltpu.VMEM((2, OROWS, OROW, LANES), F32), pltpu.VMEM((8, WIDE), F32)),
            in_specs=[any_spec] * 7,
            out_specs=(pl.BlockSpec(memory_space=pltpu.VMEM),) * 2,
            scratch_shapes=[
                pltpu.VMEM((12, NIM, COLS, LANES), BF16),
                pltpu.VMEM((NTR, NIM * COLS, LANES), F32),
                pltpu.VMEM((2, ROWS + 2, YROW, LANES), BF16),
                pltpu.VMEM((2, ROWS, MROW, LANES), F32),
                pltpu.VMEM((2, OROWS, OROW, LANES), F32),
                pltpu.VMEM((OROWS + 2, O3ROW, WIDE), BF16),
                pltpu.VMEM((2, YROW, LANES), BF16),
                pltpu.VMEM((2, YROW, LANES), BF16),
                pltpu.VMEM((512, WIDE), BF16),
                pltpu.VMEM((2, 1792, WIDE), BF16),
                pltpu.VMEM((3, 3, LANES, WIDE), BF16),
                pltpu.VMEM((3, 3, WIDE, WIDE), BF16),
                pltpu.VMEM((2, 2, LANES), F32),
                pltpu.VMEM((2, WIDE), F32),
                pltpu.VMEM((1, 2, WIDE), F32),
                pltpu.VMEM((4, 8, WIDE), F32),
                pltpu.VMEM((2, 1, WIDE), F32),
                pltpu.VMEM((2, GROUPS, 1, WIDE), F32),
                pltpu.VMEM((2, 1, 512), F32),
                pltpu.VMEM((2, GROUPS, 1, 512), F32),
                dma((ROWS,)), dma((15,)),
                *[dma((2,))] * 4, *[dma((3,))] * 2, *[dma((2,))] * 2,
                *[dma((4, GROUPS))] * 2,
            ],
            compiler_params=pltpu.CompilerParams(
                collective_id=0, has_side_effects=True, vmem_limit_bytes=VLIM),
        )(images, w_a.reshape(2, 3, 384, LANES), norm_a, w_down, norm_down, w_b.reshape(3, 3, WIDE, WIDE), norm_b)
        out = pl.pallas_call(
            result_kernel,
            out_shape=jax.ShapeDtypeStruct((OROWS, OROW, WIDE), BF16),
            in_specs=[pl.BlockSpec(memory_space=pltpu.VMEM)] * 2,
            out_specs=any_spec,
            scratch_shapes=[pltpu.VMEM((OROWS, OROW, WIDE), BF16), pltpu.VMEM((8, WIDE), F32), dma((OROWS,))],
            compiler_params=pltpu.CompilerParams(vmem_limit_bytes=6 * 1024 * 1024),
        )(z_last, coef)
        return jnp.transpose(out.reshape(OROWS, OCOLS, NIM, WIDE), (2, 0, 1, 3))

    act_spec = P(('pod', 'dp'), 'sp', None, None)
    return jax.shard_map(local_stack, mesh=mesh, in_specs=(act_spec, P(), P(), P(), P(), P(), P()), out_specs=act_spec, check_vma=False)
```

```python
import functools

import jax
import jax.numpy as jnp
from jax import lax
from jax.experimental import pallas as pl
from jax.experimental.pallas import tpu as pltpu
from jax.sharding import PartitionSpec as P

EPS_VALUE = 1e-5
F32 = jnp.float32
BF16 = jnp.bfloat16
MESH = pl.DeviceIdType.MESH

NIM = 16
ROWS = 12
COLS = 168
HALF = COLS // 2
MROW = HALF * NIM
YROW = (HALF + 1) * NIM
OROWS = 6
OCOLS = 84
OROW = OCOLS * NIM
O3ROW = (OCOLS + 2) * NIM
CHUNK = 336
NTR = 2
VLIM = 56 * 1024 * 1024
GROUPS = 8
LANES = 128
WIDE = 256
LAST, FAR_SLOT = ROWS - 1, ROWS + 1
OLAST, OFAR = OROWS - 1, OROWS + 1
FIRST = CHUNK + NIM
SUB = CHUNK // 8
PIECES = range(0, MROW, CHUNK)


def rest(m):
    lo = min(FIRST + m, MROW)
    return lo, min(CHUNK, MROW - lo)


def head(size):
    return pl.ds(0, size)


def join(parts):
    return jnp.concatenate(parts, axis=1)


def mm(lhs, rhs):
    return jnp.dot(lhs, rhs, preferred_element_type=F32)


def sublane_sum(val):
    return jnp.sum(val, axis=0)


def column_sum(val):
    return jnp.sum(val, axis=0, keepdims=True)


def kernel(x_ref, wa_ref, na_ref, wd_ref, nd_ref, wb_ref, nb_ref, z_out, c_out,
           xs, tr, yy, zz, zo, y3, yx, ys, wx, wt, wdv, wbv, nav, ndv, nbv,
           cf, st_out, st_in, sw_out, sw_in,
           x_sem, w_sem, hx_send, hx_recv, h2_send, h2_recv, h3_send, h3_recv, h4_send, h4_recv,
           st_send, st_recv):
    dp = lax.axis_index("dp")
    sp = lax.axis_index("sp")
    me = dp * 4 + sp
    upright = lax.rem(sp, 2)
    flip = 1 - upright
    near = (0, dp, sp + 2 * flip - 1)
    far = (0, dp, lax.rem(7 - sp, 4))
    has_far = jnp.logical_or(sp == 1, sp == 2)

    def x_row(r):
        return r + flip * (LAST - 2 * r)

    def tap(p):
        return p + flip * (2 - 2 * p)

    def x_slot(r):
        return {9: 1, 10: 2, 11: 10, 0: 11}.get(r, r)

    def x_copy(r):
        return pltpu.make_async_copy(x_ref.at[:, x_row(r)], xs.at[x_slot(r)], x_sem.at[r])
    wa_copies = [pltpu.make_async_copy(wa_ref.at[l, tap(p)], ys.at[l, pl.ds(384 * p, 384)], w_sem.at[3 * l + p])
                 for l in range(2) for p in range(3)]
    w_copies = [pltpu.make_async_copy(na_ref, nav, w_sem.at[6]),
                pltpu.make_async_copy(nd_ref, ndv, w_sem.at[7]),
                pltpu.make_async_copy(nb_ref, nbv, w_sem.at[8])]
    for p in range(3):
        w_copies.append(pltpu.make_async_copy(wd_ref.at[tap(p)], wdv.at[p], w_sem.at[9 + p]))
        w_copies.append(pltpu.make_async_copy(wb_ref.at[tap(p)], wbv.at[p], w_sem.at[12 + p]))

    barrier = pltpu.get_barrier_semaphore()

    def peer(k):
        x, core = sp // 2, lax.rem(sp, 2)
        x = 1 - x if k & 2 else x
        core = 1 - core if k & 1 else core
        return (0, 1 - dp if k & 4 else dp, 2 * x + core)
    for k in range(1, GROUPS):
        pl.semaphore_signal(barrier, inc=1, device_id=peer(k), device_id_type=MESH)

    for r in (1, 2):
        x_copy(r).start()
    for c in wa_copies:
        c.start()
    for r in (3, 4, 5, 6, 7, 8, 11, 0):
        x_copy(r).start()

    def halo(src_near, dst_near, src_far, dst_far, send, recv):
        n_copy = pltpu.make_async_remote_copy(
            src_ref=src_near, dst_ref=dst_near, send_sem=send.at[0], recv_sem=recv.at[0],
            device_id=near, device_id_type=MESH)
        f_copy = pltpu.make_async_remote_copy(
            src_ref=src_far, dst_ref=dst_far, send_sem=send.at[1], recv_sem=recv.at[1],
            device_id=far, device_id_type=MESH)
        return n_copy, f_copy

    hx_near, hx_far = halo(x_ref.at[:, x_row(0)], xs.at[0], x_ref.at[:, x_row(LAST)], xs.at[9],
                           hx_send, hx_recv)
    h2_near, h2_far = halo(yy.at[:, 1], yy.at[:, 0], yy.at[:, ROWS], yy.at[:, FAR_SLOT], h2_send, h2_recv)
    h3_near, hy0 = halo(yy.at[:, 1], yy.at[:, FAR_SLOT], ys.at[0], yx.at[0], h3_send, h3_recv)
    hy1 = pltpu.make_async_remote_copy(
        src_ref=ys.at[1], dst_ref=yx.at[1], send_sem=h3_send.at[2], recv_sem=h3_recv.at[2],
        device_id=far, device_id_type=MESH)
    h4_near, h4_far = halo(y3.at[1], y3.at[0], y3.at[OROWS], y3.at[OFAR], h4_send, h4_recv)

    zpad = jnp.zeros((NIM, LANES), BF16)

    @pl.loop(0, ROWS + 2)
    def _(r):
        yy[0, r, head(NIM), :] = zpad
        yy[1, r, pl.ds(HALF * NIM, NIM), :] = zpad


    @pl.loop(0, OROWS + 2)
    def _(r):
        for c in (0, OCOLS + 1):
            y3[r, pl.ds(c * NIM, NIM), :] = jnp.zeros((NIM, WIDE), BF16)

    @pl.when(jnp.logical_not(has_far))
    def _():
        for b in range(2):
            yy[b, FAR_SLOT] = jnp.zeros((YROW, LANES), BF16)
        y3[OFAR] = jnp.zeros((O3ROW, WIDE), BF16)

    def transpose_piece(r, lo, hi, slot, src):
        for n in range(NIM):
            tr[slot, pl.ds(n * COLS + lo, hi - lo), :] = xs[src, n, pl.ds(lo, hi - lo), :].astype(F32)
        for j in range(lo, hi):
            v = tr[slot, pl.ds(j, NIM, stride=COLS), :].astype(BF16)
            b, a = (j + 1) % 2, (j + 1) // 2
            yy[b, r, pl.ds(a * NIM, NIM), :] = v

    def transpose_row(r, src):
        transpose_piece(r, 0, COLS, 0, src)

    with jax.named_scope('transpose'):
        @pl.loop(1, 3)
        def _(r):
            pltpu.make_async_copy(x_ref.at[:, x_row(r)], xs.at[r], x_sem.at[r]).wait()
            transpose_row(r + 1, r)
    for r in (9, 10):
        x_copy(r).start()

    with jax.named_scope('barrier'):
        pl.semaphore_wait(barrier, GROUPS - 1)

    @pl.when(has_far)
    def _():
        hx_far.start()
    hx_near.start()

    for c in wa_copies:
        c.wait()
    zblk = jnp.zeros((LANES, LANES), BF16)

    def tile(layer, p, q):
        return zblk if q is None else ys[layer, pl.ds(384 * p + LANES * q, LANES), :]

    for layer in range(2):
        def put(k, lo, hi):
            wt[layer, pl.ds(k, LANES), head(LANES)] = tile(layer, *lo)
            wt[layer, pl.ds(k, LANES), pl.ds(LANES, LANES)] = tile(layer, *hi)
        for q in range(3):
            put(WIDE * q, (1, q), (0, q))
            put(WIDE * q + LANES, (2, q), (1, q))
        for e, p in enumerate((0, 2)):
            k = 768 + 512 * e
            put(k, (p, 0), (p, None))
            put(k + LANES, (p, 1), (p, 0))
            put(k + WIDE, (p, 2), (p, 1))
            put(k + 384, (p, None), (p, 2))
    for k, (lo, hi) in enumerate(((0, None), (1, 0), (2, 1), (None, 2))):
        wx[pl.ds(LANES * k, LANES), head(LANES)] = tile(1, 1, lo)
        wx[pl.ds(LANES * k, LANES), pl.ds(LANES, LANES)] = tile(1, 1, hi)

    ys[0, head(NIM), :] = zpad
    ys[1, pl.ds(HALF * NIM, NIM), :] = zpad

    with jax.named_scope('transpose2'):
        @pl.loop(3, 5)
        def _(r):
            pltpu.make_async_copy(x_ref.at[:, x_row(r)], xs.at[r], x_sem.at[r]).wait()
            transpose_row(r + 1, r)
    for r in (5, 6, 7, 8, 11, 0, 9, 10):
        x_copy(r).wait()
    for c in w_copies:
        c.start()

    def exchange(layer, rows, meanwhile=None):
        out, slots = (st_out, st_in) if layer < 2 else (sw_out, sw_in)
        at = layer % 2
        buf = join(rows)
        out[at] = buf
        slots[at, me] = buf
        copies = []
        for k in (7, 6, 5, 4, 3, 2, 1):
            copies.append(pltpu.make_async_remote_copy(
                src_ref=out.at[at], dst_ref=slots.at[at, me],
                send_sem=st_send.at[layer, k], recv_sem=st_recv.at[layer, k],
                device_id=peer(k), device_id_type=MESH))
        for c in copies:
            c.start()
        if meanwhile is not None:
            meanwhile()
        with jax.named_scope(f'stat{layer}'):
            for c in copies:
                c.wait_recv()
        total = slots[at, 0]
        for s in range(1, GROUPS):
            total = total + slots[at, s]

        def finish():
            for c in copies:
                c.wait_send()
        half = total.shape[1] // 2
        return total[:, :half], total[:, half:], finish

    def moments(s1, s2, count):
        mean = s1 / count
        var = s2 / count - mean * mean
        return mean, lax.rsqrt(var + EPS_VALUE)

    def normalise(z, mean, inv, gamma, beta):
        return jnp.maximum(gamma * (z - mean) * inv + beta, 0.0).astype(BF16)

    TAPS = (((0, 0), (1, 0), (0, NIM)), ((1, 0), (0, NIM), (1, NIM)))
    QUAD = ((0, 0), (1, 0), (0, NIM), (1, NIM))

    def pair_layer(layer, ahead, near_row, far_row, meanwhile=None):
        def conv(i, carry, work=None):
            s1, s2 = carry
            for m in PIECES:
                if work is not None:
                    work(i, m // CHUNK)
                def take(taps, rows):
                    return join(
                        [yy[plane, i + rr, pl.ds(m + off, CHUNK), :] for plane, off in taps for rr in rows])
                mid = [mm(take(TAPS[b], (1, 2)), wt[layer, head(768), :])
                       for b in range(2)]
                edge = [mm(take(QUAD, (3 * e,)), wt[layer, pl.ds(768 + 512 * e, 512), :]) for e in range(2)]
                for b in range(2):
                    for e in range(2):
                        z = mid[b][:, LANES * e:LANES * e + LANES] + edge[e][:, LANES * b:LANES * b + LANES]
                        zz[b, i + e, pl.ds(m, CHUNK), :] = z
                        z8 = z.reshape(SUB, 8, LANES)
                        s1 = s1 + sublane_sum(z8)
                        s2 = s2 + sublane_sum(z8 * z8)
            return s1, s2

        def border(it, carry):
            @pl.when(it == 0)
            def _():
                near_row.wait_recv()

            @pl.when(jnp.logical_and(it == 1, has_far))
            def _():
                far_row.wait_recv()
            if layer == 0:
                @pl.when(jnp.logical_or(it == 0, has_far))
                def _():
                    transpose_row(it * (FAR_SLOT), it * 9)
            return conv(10 * it, carry)

        zero = jnp.zeros((8, LANES), F32)
        carry = (zero, zero)
        with jax.named_scope(f'pairA{layer}'):
            for i in (2, 4, 6, 8):
                carry = conv(i, carry, ahead)
        if layer == 1:
            @pl.when(sp == 2)
            def _():
                hy0.start()
        with jax.named_scope(f'pairB{layer}'):
            s1, s2 = lax.fori_loop(0, 2, border, carry)
        s1, s2, finish = exchange(layer, [column_sum(s1), column_sum(s2)],
                                  meanwhile)
        mean, inv = moments(s1, s2, float(32 * 48 * 168))
        return mean, inv, finish

    def norm_piece(r, m, size, coef, slot=None, copy_too=False):
        if size == 0:
            return
        par = load_coef(coef)
        slot = r + 1 if slot is None else slot
        for b, plane, off in ((0, 1, m), (1, 0, NIM + m)):
            val = normalise(zz[b, r, pl.ds(m, size), :], *par)
            yy[plane, slot, pl.ds(off, size), :] = val
            if copy_too:
                ys[plane, pl.ds(off, size), :] = val

    def norm_row(r, coef):
        norm_piece(r, 0, MROW, coef)

    def save_coef(slot, width, mean, inv, gamma, beta):
        for k, v in enumerate((mean, inv, gamma, beta)):
            cf[slot, k:k + 1, head(width)] = v
        return slot

    def load_coef(slot, lane=0):
        return [cf[slot, k:k + 1, pl.ds(lane, LANES)] for k in range(4)]

    def first_ahead(i, c):
        for e in range(2):
            r = i + 3 + e if i < 8 else (LAST) * (1 - e)
            transpose_piece(r + 1, 48 * c, min(48 * c + 48, COLS), e % NTR, x_slot(r))

    mean, inv, fin1 = pair_layer(0, first_ahead, hx_near, hx_far)
    for c in w_copies:
        c.wait()
    coef1 = save_coef(0, LANES, mean, inv, nav[0, 0:1], nav[0, 1:2])

    with jax.named_scope('norm1'):
        norm_row(LAST, coef1)

        @pl.when(has_far)
        def _():
            h2_far.start()
        norm_row(0, coef1)
        h2_near.start()

        @pl.loop(1, 5)
        def _(r):
            norm_piece(r, 0, FIRST, coef1)

    def second_ahead(i, c):
        if i == 2:
            for r in range(1, 5):
                norm_piece(r, *rest(c * CHUNK), coef1)
        if i < 8:
            for r in (i + 3, i + 4):
                if r < LAST:
                    norm_piece(r, c * CHUNK, CHUNK, coef1, None, r == ROWS - 2)

    def lone_row(m, taps):
        res = None
        for p in taps:
            src = (yy.at[:, ROWS], yy.at[:, FAR_SLOT], yx)[p]
            lhs = join([src[plane, pl.ds(m + off, CHUNK), :] for plane, off in QUAD])
            w_val = wx[...] if p == 1 else wt[1, pl.ds(768 + WIDE * p, 512), :]
            part = mm(lhs, w_val)
            res = part if res is None else res + part
        return res

    def second_meanwhile():
        @pl.when(sp == 2)
        def _():
            hy1.start()

        @pl.when(sp == 1)
        def _():
            for m in PIECES:
                res = lone_row(m, (0, 1))
                tr[0, pl.ds(m, CHUNK), :] = res[:, :LANES]
                tr[1, pl.ds(m, CHUNK), :] = res[:, LANES:]

    mean2, inv2, fin2 = pair_layer(1, second_ahead, h2_near, h2_far, second_meanwhile)
    coef2 = save_coef(1, LANES, mean2, inv2, nav[1, 0:1], nav[1, 1:2])
    h2_near.wait_send()

    @pl.when(has_far)
    def _():
        h2_far.wait_send()

    sends_near = upright == 1
    with jax.named_scope('norm2'):
        norm_piece(flip, 0, MROW, coef2, 1)

        @pl.when(sends_near)
        def _():
            h3_near.start()
        for r in (1, 2):
            norm_piece(r + flip, 0, FIRST, coef2, r + 1)

    wd_taps = ((1, 0), (0, NIM), (1, NIM))

    def wide_conv(dst, i, lhs_of, w_val, carry, work=None):
        s1, s2 = carry
        for m in PIECES:
            if work is not None:
                work(m)
            lhs = join(lhs_of(m))
            res = mm(lhs, w_val)
            dst[0, i, pl.ds(m, CHUNK), :] = res[:, :LANES]
            dst[1, i, pl.ds(m, CHUNK), :] = res[:, LANES:]
            r3 = res.reshape(SUB, 8, WIDE)
            s1 = s1 + sublane_sum(r3)
            s2 = s2 + sublane_sum(r3 * r3)
        return s1, s2

    def wide_stats(layer, carry):
        s1, s2 = carry
        s1, s2, finish = exchange(layer, [column_sum(s1), column_sum(s2)])
        mean, inv = moments(s1, s2, float(32 * 24 * 84))
        return mean, inv, finish

    zero = jnp.zeros((8, WIDE), F32)

    def down_lhs(slots):
        return lambda m: [yy[plane, slot, pl.ds(m + off, CHUNK), :] for slot in slots for plane, off in wd_taps]

    wd_val = wdv[...].reshape(9 * LANES, WIDE)

    def down_ahead(it):
        def work(m):
            if it == 0:
                for r in (1, 2):
                    norm_piece(r + flip, *rest(m), coef2, r + 1)
            if it < 4:
                for e in range(2):
                    norm_piece(2 * it + 3 + e + flip, m, CHUNK, coef2, 2 * it + 4 + e)
            else:
                norm_piece(LAST * upright, m, CHUNK, coef2, ROWS)
        return work

    with jax.named_scope('wide2'):
        carry = (zero, zero)
        for it in range(OLAST):
            carry = wide_conv(zo, it, down_lhs((2 * it + 1, 2 * it + 2, 2 * it + 3)), wd_val, carry, down_ahead(it))

    with jax.named_scope('halo2'):
        @pl.when(sp == 1)
        def _():
            hy0.wait_recv()
            hy1.wait_recv()

            par = load_coef(coef2)
            for m in PIECES:
                res = lone_row(m, (2,))
                for b, plane, off in ((0, 1, m), (1, 0, NIM + m)):
                    z = tr[b, pl.ds(m, CHUNK), :] + res[:, LANES * b:LANES * b + LANES]
                    yy[plane, FAR_SLOT, pl.ds(off, CHUNK), :] = normalise(z, *par)


        @pl.when(flip == 1)
        def _():
            h3_near.wait_recv()
    with jax.named_scope('wide2B'):
        slots = (LAST + 2 * flip, ROWS, FAR_SLOT - ROWS * flip)
        carry = wide_conv(zo, OLAST, down_lhs(slots), wd_val, carry)
    mean3, inv3, fin3 = wide_stats(2, carry)
    coef3 = save_coef(2, WIDE, mean3, inv3, ndv[0:1], ndv[1:2])

    def norm3_piece(r, m, size):
        if size == 0:
            return
        step = lax.rem(r - flip + OROWS, OROWS)
        for h in range(2):
            par = load_coef(coef3, LANES * h)
            y3[r + 1, pl.ds(NIM + m, size), pl.ds(LANES * h, LANES)] = normalise(zo[h, step, pl.ds(m, size), :], *par)

    def norm3(r):
        norm3_piece(r, 0, OROW)

    with jax.named_scope('norm3'):
        norm3(OLAST)

        @pl.when(has_far)
        def _():
            h4_far.start()

        norm3(0)
        h4_near.start()

        @pl.loop(1, 3)
        def _(r):
            norm3_piece(r, 0, FIRST)

    def last_lhs(i, taps=(0, 1, 2)):
        return lambda m: [y3[i + p, pl.ds(m + NIM * q, CHUNK), :] for p in taps for q in range(3)]

    wb_val = wbv[...].reshape(9 * WIDE, WIDE)

    def last_ahead(it):
        def work(m):
            if it == 1:
                for r in range(1, 3):
                    norm3_piece(r, *rest(m))
                norm3_piece(3, m, CHUNK)
            elif it == 2:
                norm3_piece(4, m, CHUNK)
        return work

    with jax.named_scope('wide3A'):
        carry = (zero, zero)
        for it in (1, 2, 3, 4):
            carry = wide_conv(z_out, it, last_lhs(it), wb_val, carry, last_ahead(it))
    with jax.named_scope('wide3B'):
        with jax.named_scope('near3'):
            h4_near.wait_recv()
        carry = wide_conv(z_out, 0, last_lhs(0), wb_val, carry)
        part_w = wbv[head(2)].reshape(6 * WIDE, WIDE)
        last_w = wbv[2].reshape(3 * WIDE, WIDE)
        r = OLAST
        for m in PIECES:
            res = mm(join(last_lhs(r, (0, 1))(m)), part_w)
            z_out[0, r, pl.ds(m, CHUNK), :] = res[:, :LANES]
            z_out[1, r, pl.ds(m, CHUNK), :] = res[:, LANES:]
        with jax.named_scope('far3'):
            @pl.when(has_far)
            def _():
                h4_far.wait_recv()
        s1, s2 = carry
        for m in PIECES:
            res = mm(join(last_lhs(r, (2,))(m)), last_w)
            res = res + join([z_out[h, r, pl.ds(m, CHUNK), :] for h in range(2)])
            z_out[0, r, pl.ds(m, CHUNK), :] = res[:, :LANES]
            z_out[1, r, pl.ds(m, CHUNK), :] = res[:, LANES:]
            r3 = res.reshape(SUB, 8, WIDE)
            s1 = s1 + sublane_sum(r3)
            s2 = s2 + sublane_sum(r3 * r3)
        carry = s1, s2
    mean4, inv4, fin4 = wide_stats(3, carry)
    for k, v in enumerate((mean4, inv4, nbv[0, 0:1], nbv[0, 1:2])):
        c_out[k:k + 1] = v

    with jax.named_scope('drain'):
        hx_near.wait_send()
        h4_near.wait_send()

        @pl.when(has_far)
        def _():
            hx_far.wait_send()
            h4_far.wait_send()

        @pl.when(sends_near)
        def _():
            h3_near.wait_send()

        @pl.when(sp == 2)
        def _():
            hy0.wait_send()
            hy1.wait_send()
        for f in (fin1, fin2, fin3, fin4):
            f()


def result_kernel(z_ref, c_ref, out_ref, yo, cf, sem):
    flip = 1 - lax.rem(lax.axis_index("sp"), 2)

    def copy(r):
        return pltpu.make_async_copy(yo.at[r], out_ref.at[r + flip * (OLAST - 2 * r)], sem.at[r])

    mean, inv, gamma, beta = [c_ref[k:k + 1] for k in range(4)]
    scale = gamma * inv
    cf[0:1] = scale
    cf[1:2] = beta - mean * scale
    small = jnp.logical_and(jnp.max(jnp.abs(scale)) < 1e15, jnp.max(jnp.abs(mean)) < 1e20)

    @pl.when(small)
    def _():
        @pl.loop(0, OROWS)
        def _(r):
            for h in range(2):
                lanes = pl.ds(LANES * h, LANES)
                y = z_ref[h, r] * cf[0:1, lanes] + cf[1:2, lanes]
                yo[r, :, lanes] = jnp.maximum(y, 0.0).astype(BF16)
            copy(r).start()

    @pl.when(jnp.logical_not(small))
    def _():
        @pl.loop(0, OROWS)
        def _(r):
            for h in range(2):
                lanes = pl.ds(LANES * h, LANES)
                mean, inv, gamma, beta = [c_ref[k:k + 1, lanes] for k in range(4)]
                yo[r, :, lanes] = jnp.maximum(gamma * (z_ref[h, r] - mean) * inv + beta, 0.0).astype(BF16)
            copy(r).start()

    @pl.loop(0, OROWS)
    def _(r):
        copy(r).wait()


def solution(mesh):
    any_spec = pl.BlockSpec(memory_space=pl.ANY)
    dma = pltpu.SemaphoreType.DMA

    def local_stack(images, w_a, norm_a, w_down, norm_down, w_b, norm_b):
        z_last, coef = pl.pallas_call(
            kernel,
            out_shape=(pltpu.VMEM((2, OROWS, OROW, LANES), F32), pltpu.VMEM((8, WIDE), F32)),
            in_specs=[any_spec] * 7,
            out_specs=(pl.BlockSpec(memory_space=pltpu.VMEM),) * 2,
            scratch_shapes=[
                pltpu.VMEM((12, NIM, COLS, LANES), BF16),
                pltpu.VMEM((NTR, NIM * COLS, LANES), F32),
                pltpu.VMEM((2, ROWS + 2, YROW, LANES), BF16),
                pltpu.VMEM((2, ROWS, MROW, LANES), F32),
                pltpu.VMEM((2, OROWS, OROW, LANES), F32),
                pltpu.VMEM((OROWS + 2, O3ROW, WIDE), BF16),
                pltpu.VMEM((2, YROW, LANES), BF16),
                pltpu.VMEM((2, YROW, LANES), BF16),
                pltpu.VMEM((512, WIDE), BF16),
                pltpu.VMEM((2, 1792, WIDE), BF16),
                pltpu.VMEM((3, 3, LANES, WIDE), BF16),
                pltpu.VMEM((3, 3, WIDE, WIDE), BF16),
                pltpu.VMEM((2, 2, LANES), F32),
                pltpu.VMEM((2, WIDE), F32),
                pltpu.VMEM((1, 2, WIDE), F32),
                pltpu.VMEM((4, 8, WIDE), F32),
                pltpu.VMEM((2, 1, WIDE), F32),
                pltpu.VMEM((2, GROUPS, 1, WIDE), F32),
                pltpu.VMEM((2, 1, 512), F32),
                pltpu.VMEM((2, GROUPS, 1, 512), F32),
                dma((ROWS,)), dma((15,)),
                *[dma((2,))] * 4, *[dma((3,))] * 2, *[dma((2,))] * 2,
                *[dma((4, GROUPS))] * 2,
            ],
            compiler_params=pltpu.CompilerParams(
                collective_id=0, has_side_effects=True, vmem_limit_bytes=VLIM),
        )(images, w_a.reshape(2, 3, 384, LANES), norm_a, w_down, norm_down, w_b.reshape(3, 3, WIDE, WIDE), norm_b)
        out = pl.pallas_call(
            result_kernel,
            out_shape=jax.ShapeDtypeStruct((OROWS, OROW, WIDE), BF16),
            in_specs=[pl.BlockSpec(memory_space=pltpu.VMEM)] * 2,
            out_specs=any_spec,
            scratch_shapes=[pltpu.VMEM((OROWS, OROW, WIDE), BF16), pltpu.VMEM((8, WIDE), F32), dma((OROWS,))],
            compiler_params=pltpu.CompilerParams(vmem_limit_bytes=6 * 1024 * 1024),
        )(z_last, coef)
        return jnp.transpose(out.reshape(OROWS, OCOLS, NIM, WIDE), (2, 0, 1, 3))

    act_spec = P(('pod', 'dp'), 'sp', None, None)
    return jax.shard_map(local_stack, mesh=mesh, in_specs=(act_spec, P(), P(), P(), P(), P(), P()), out_specs=act_spec, check_vma=False)
```

```python
import functools

import jax
import jax.numpy as jnp
from jax import lax
from jax.experimental import pallas as pl
from jax.experimental.pallas import tpu as pltpu
from jax.sharding import PartitionSpec as P

EPS_VALUE = 1e-5
F32 = jnp.float32
BF16 = jnp.bfloat16
MESH = pl.DeviceIdType.MESH

NIM = 16
ROWS = 12
COLS = 168
HALF = COLS // 2
MROW = HALF * NIM
YROW = (HALF + 1) * NIM
OROWS = 6
OCOLS = 84
OROW = OCOLS * NIM
O3ROW = (OCOLS + 2) * NIM
CHUNK = 336
NTR = 2
VLIM = 56 * 1024 * 1024
GROUPS = 8
LANES = 128
WIDE = 256
LAST, FAR_SLOT = ROWS - 1, ROWS + 1
OLAST, OFAR = OROWS - 1, OROWS + 1
FIRST = CHUNK + NIM
SUB = CHUNK // 8
PIECES = range(0, MROW, CHUNK)


def rest(m):
    lo = min(FIRST + m, MROW)
    return lo, min(CHUNK, MROW - lo)


def head(size):
    return pl.ds(0, size)


def join(parts):
    return jnp.concatenate(parts, axis=1)


def mm(lhs, rhs):
    return jnp.dot(lhs, rhs, preferred_element_type=F32)


def sublane_sum(val):
    return jnp.sum(val, axis=0)


def column_sum(val):
    return jnp.sum(val, axis=0, keepdims=True)


def kernel(x_ref, wa_ref, na_ref, wd_ref, nd_ref, wb_ref, nb_ref, z_out, c_out,
           xs, yy, zz, zo, y3, yx, ys, wx, wt, wdv, wbv, nav, ndv, nbv,
           cf, st_out, st_in, sw_out, sw_in,
           x_sem, w_sem, hx_send, hx_recv, h2_send, h2_recv, h3_send, h3_recv, h4_send, h4_recv,
           st_send, st_recv):
    dp = lax.axis_index("dp")
    sp = lax.axis_index("sp")
    me = dp * 4 + sp
    upright = lax.rem(sp, 2)
    flip = 1 - upright
    near = (0, dp, sp + 2 * flip - 1)
    far = (0, dp, lax.rem(7 - sp, 4))
    has_far = jnp.logical_or(sp == 1, sp == 2)

    def x_row(r):
        return r + flip * (LAST - 2 * r)

    def tap(p):
        return p + flip * (2 - 2 * p)

    def x_slot(r):
        return {9: 1, 10: 2, 11: 10, 0: 11}.get(r, r)

    def x_copy(r):
        return pltpu.make_async_copy(x_ref.at[:, x_row(r)], xs.at[x_slot(r)], x_sem.at[r])
    wa_copies = [pltpu.make_async_copy(wa_ref.at[l, tap(p)], ys.at[l, pl.ds(384 * p, 384)], w_sem.at[3 * l + p])
                 for l in range(2) for p in range(3)]
    w_copies = [pltpu.make_async_copy(na_ref, nav, w_sem.at[6]),
                pltpu.make_async_copy(nd_ref, ndv, w_sem.at[7]),
                pltpu.make_async_copy(nb_ref, nbv, w_sem.at[8])]
    for p in range(3):
        w_copies.append(pltpu.make_async_copy(wd_ref.at[tap(p)], wdv.at[p], w_sem.at[9 + p]))
        w_copies.append(pltpu.make_async_copy(wb_ref.at[tap(p)], wbv.at[p], w_sem.at[12 + p]))

    barrier = pltpu.get_barrier_semaphore()

    def peer(k):
        x, core = sp // 2, lax.rem(sp, 2)
        x = 1 - x if k & 2 else x
        core = 1 - core if k & 1 else core
        return (0, 1 - dp if k & 4 else dp, 2 * x + core)
    for k in range(1, GROUPS):
        pl.semaphore_signal(barrier, inc=1, device_id=peer(k), device_id_type=MESH)

    for r in (1, 2):
        x_copy(r).start()
    for c in wa_copies:
        c.start()
    for r in (3, 4, 5, 6, 7, 8, 11, 0):
        x_copy(r).start()

    def halo(src_near, dst_near, src_far, dst_far, send, recv):
        n_copy = pltpu.make_async_remote_copy(
            src_ref=src_near, dst_ref=dst_near, send_sem=send.at[0], recv_sem=recv.at[0],
            device_id=near, device_id_type=MESH)
        f_copy = pltpu.make_async_remote_copy(
            src_ref=src_far, dst_ref=dst_far, send_sem=send.at[1], recv_sem=recv.at[1],
            device_id=far, device_id_type=MESH)
        return n_copy, f_copy

    hx_near, hx_far = halo(x_ref.at[:, x_row(0)], xs.at[0], x_ref.at[:, x_row(LAST)], xs.at[9],
                           hx_send, hx_recv)
    h2_near, h2_far = halo(yy.at[:, 1], yy.at[:, 0], yy.at[:, ROWS], yy.at[:, FAR_SLOT], h2_send, h2_recv)
    h3_near, hy0 = halo(yy.at[:, 1], yy.at[:, FAR_SLOT], ys.at[0], yx.at[0], h3_send, h3_recv)
    hy1 = pltpu.make_async_remote_copy(
        src_ref=ys.at[1], dst_ref=yx.at[1], send_sem=h3_send.at[2], recv_sem=h3_recv.at[2],
        device_id=far, device_id_type=MESH)
    h4_near, h4_far = halo(y3.at[1], y3.at[0], y3.at[OROWS], y3.at[OFAR], h4_send, h4_recv)

    zpad = jnp.zeros((NIM, LANES), BF16)

    @pl.loop(0, ROWS + 2)
    def _(r):
        yy[0, r, head(NIM), :] = zpad
        yy[1, r, pl.ds(HALF * NIM, NIM), :] = zpad


    @pl.loop(0, OROWS + 2)
    def _(r):
        for c in (0, OCOLS + 1):
            y3[r, pl.ds(c * NIM, NIM), :] = jnp.zeros((NIM, WIDE), BF16)

    @pl.when(jnp.logical_not(has_far))
    def _():
        xs[9] = jnp.zeros((NIM, COLS, LANES), BF16)
        y3[OFAR] = jnp.zeros((O3ROW, WIDE), BF16)

    def transpose_piece(r, lo, hi, slot, src):
        for n in range(NIM):
            zo[slot, pl.ds(n * COLS + lo, hi - lo), :] = xs[src, n, pl.ds(lo, hi - lo), :].astype(F32)
        for j in range(lo, hi):
            v = zo[slot, pl.ds(j, NIM, stride=COLS), :].astype(BF16)
            b, a = (j + 1) % 2, (j + 1) // 2
            yy[b, r, pl.ds(a * NIM, NIM), :] = v

    def transpose_row(r, src):
        transpose_piece(r, 0, COLS, 0, src)

    with jax.named_scope('transpose'):
        @pl.loop(1, 3)
        def _(r):
            pltpu.make_async_copy(x_ref.at[:, x_row(r)], xs.at[r], x_sem.at[r]).wait()
            transpose_row(r + 1, r)
    for r in (9, 10):
        x_copy(r).start()

    with jax.named_scope('barrier'):
        pl.semaphore_wait(barrier, GROUPS - 1)

    @pl.when(has_far)
    def _():
        hx_far.start()
    hx_near.start()

    for c in wa_copies:
        c.wait()
    zblk = jnp.zeros((LANES, LANES), BF16)

    def tile(layer, p, q):
        return zblk if q is None else ys[layer, pl.ds(384 * p + LANES * q, LANES), :]

    for layer in range(2):
        def put(k, lo, hi):
            wt[layer, pl.ds(k, LANES), head(LANES)] = tile(layer, *lo)
            wt[layer, pl.ds(k, LANES), pl.ds(LANES, LANES)] = tile(layer, *hi)
        for q in range(3):
            put(WIDE * q, (1, q), (0, q))
            put(WIDE * q + LANES, (2, q), (1, q))
        for e, p in enumerate((0, 2)):
            k = 768 + 512 * e
            put(k, (p, 0), (p, None))
            put(k + LANES, (p, 1), (p, 0))
            put(k + WIDE, (p, 2), (p, 1))
            put(k + 384, (p, None), (p, 2))
    for k, (lo, hi) in enumerate(((0, None), (1, 0), (2, 1), (None, 2))):
        wx[pl.ds(LANES * k, LANES), head(LANES)] = tile(1, 1, lo)
        wx[pl.ds(LANES * k, LANES), pl.ds(LANES, LANES)] = tile(1, 1, hi)

    ys[0, head(NIM), :] = zpad
    ys[1, pl.ds(HALF * NIM, NIM), :] = zpad

    with jax.named_scope('transpose2'):
        @pl.loop(3, 5)
        def _(r):
            pltpu.make_async_copy(x_ref.at[:, x_row(r)], xs.at[r], x_sem.at[r]).wait()
            transpose_row(r + 1, r)
    for r in (5, 6, 7, 8, 11, 0, 9, 10):
        x_copy(r).wait()
    for c in w_copies:
        c.start()

    def exchange(layer, rows, meanwhile=None):
        out, slots = (st_out, st_in) if layer < 2 else (sw_out, sw_in)
        at = layer % 2
        buf = join(rows)
        out[at] = buf
        slots[at, me] = buf
        copies = []
        for k in (7, 6, 5, 4, 3, 2, 1):
            copies.append(pltpu.make_async_remote_copy(
                src_ref=out.at[at], dst_ref=slots.at[at, me],
                send_sem=st_send.at[layer, k], recv_sem=st_recv.at[layer, k],
                device_id=peer(k), device_id_type=MESH))
        for c in copies:
            c.start()
        if meanwhile is not None:
            meanwhile()
        with jax.named_scope(f'stat{layer}'):
            for c in copies:
                c.wait_recv()
        total = slots[at, 0]
        for s in range(1, GROUPS):
            total = total + slots[at, s]

        def finish():
            for c in copies:
                c.wait_send()
        half = total.shape[1] // 2
        return total[:, :half], total[:, half:], finish

    def moments(s1, s2, count):
        mean = s1 / count
        var = s2 / count - mean * mean
        return mean, lax.rsqrt(var + EPS_VALUE)

    def normalise(z, mean, inv, gamma, beta):
        return jnp.maximum(gamma * (z - mean) * inv + beta, 0.0).astype(BF16)

    TAPS = (((0, 0), (1, 0), (0, NIM)), ((1, 0), (0, NIM), (1, NIM)))
    QUAD = ((0, 0), (1, 0), (0, NIM), (1, NIM))

    def pair_layer(layer, ahead, near_row, far_row, meanwhile=None):
        def conv(i, carry, work=None):
            s1, s2 = carry
            for m in PIECES:
                if work is not None:
                    work(i, m // CHUNK)
                def take(taps, rows):
                    return join(
                        [yy[plane, i + rr, pl.ds(m + off, CHUNK), :] for plane, off in taps for rr in rows])
                mid = [mm(take(TAPS[b], (1, 2)), wt[layer, head(768), :])
                       for b in range(2)]
                edge = [mm(take(QUAD, (3 * e,)), wt[layer, pl.ds(768 + 512 * e, 512), :]) for e in range(2)]
                for b in range(2):
                    for e in range(2):
                        z = mid[b][:, LANES * e:LANES * e + LANES] + edge[e][:, LANES * b:LANES * b + LANES]
                        zz[b, i + e, pl.ds(m, CHUNK), :] = z
                        z8 = z.reshape(SUB, 8, LANES)
                        s1 = s1 + sublane_sum(z8)
                        s2 = s2 + sublane_sum(z8 * z8)
            return s1, s2

        def border(it, carry):
            @pl.when(it == 0)
            def _():
                near_row.wait_recv()

            @pl.when(jnp.logical_and(it == 1, has_far))
            def _():
                far_row.wait_recv()

            def halo_ahead(i, c):
                transpose_piece(it * FAR_SLOT, 48 * c, min(48 * c + 48, COLS), c % NTR, it * 9)
            return conv(10 * it, carry, halo_ahead if layer == 0 else None)

        zero = jnp.zeros((8, LANES), F32)
        carry = (zero, zero)
        with jax.named_scope(f'pairA{layer}'):
            for i in (2, 4, 6, 8):
                carry = conv(i, carry, ahead)
        if layer == 1:
            @pl.when(sp == 2)
            def _():
                hy0.start()
        with jax.named_scope(f'pairB{layer}'):
            s1, s2 = lax.fori_loop(0, 2, border, carry)
        s1, s2, finish = exchange(layer, [column_sum(s1), column_sum(s2)],
                                  meanwhile)
        mean, inv = moments(s1, s2, float(32 * 48 * 168))
        return mean, inv, finish

    def norm_piece(r, m, size, coef, slot=None, copy_too=False):
        if size == 0:
            return
        par = load_coef(coef)
        slot = r + 1 if slot is None else slot
        for b, plane, off in ((0, 1, m), (1, 0, NIM + m)):
            val = normalise(zz[b, r, pl.ds(m, size), :], *par)
            yy[plane, slot, pl.ds(off, size), :] = val
            if copy_too:
                ys[plane, pl.ds(off, size), :] = val

    def norm_row(r, coef):
        norm_piece(r, 0, MROW, coef)

    def save_coef(slot, width, mean, inv, gamma, beta):
        for k, v in enumerate((mean, inv, gamma, beta)):
            cf[slot, k:k + 1, head(width)] = v
        return slot

    def load_coef(slot, lane=0):
        return [cf[slot, k:k + 1, pl.ds(lane, LANES)] for k in range(4)]

    def first_ahead(i, c):
        for e in range(2):
            r = i + 3 + e if i < 8 else (LAST) * (1 - e)
            transpose_piece(r + 1, 48 * c, min(48 * c + 48, COLS), e % NTR, x_slot(r))

    mean, inv, fin1 = pair_layer(0, first_ahead, hx_near, hx_far)
    for c in w_copies:
        c.wait()
    coef1 = save_coef(0, LANES, mean, inv, nav[0, 0:1], nav[0, 1:2])

    with jax.named_scope('norm1'):
        norm_row(LAST, coef1)

        @pl.when(has_far)
        def _():
            h2_far.start()
        norm_row(0, coef1)
        h2_near.start()

        @pl.loop(1, 5)
        def _(r):
            norm_piece(r, 0, FIRST, coef1)

    def second_ahead(i, c):
        if i == 2:
            for r in range(1, 5):
                norm_piece(r, *rest(c * CHUNK), coef1)
        if i < 8:
            for r in (i + 3, i + 4):
                if r < LAST:
                    norm_piece(r, c * CHUNK, CHUNK, coef1, None, r == ROWS - 2)

    def lone_row(m, taps):
        res = None
        for p in taps:
            src = (yy.at[:, ROWS], yy.at[:, FAR_SLOT], yx)[p]
            lhs = join([src[plane, pl.ds(m + off, CHUNK), :] for plane, off in QUAD])
            w_val = wx[...] if p == 1 else wt[1, pl.ds(768 + WIDE * p, 512), :]
            part = mm(lhs, w_val)
            res = part if res is None else res + part
        return res

    def second_meanwhile():
        @pl.when(sp == 2)
        def _():
            hy1.start()

        @pl.when(sp == 1)
        def _():
            for m in PIECES:
                res = lone_row(m, (0, 1))
                zo[0, pl.ds(OLAST * OROW + m, CHUNK), :] = res[:, :LANES]
                zo[1, pl.ds(OLAST * OROW + m, CHUNK), :] = res[:, LANES:]

    mean2, inv2, fin2 = pair_layer(1, second_ahead, h2_near, h2_far, second_meanwhile)
    coef2 = save_coef(1, LANES, mean2, inv2, nav[1, 0:1], nav[1, 1:2])
    h2_near.wait_send()

    @pl.when(has_far)
    def _():
        h2_far.wait_send()

    sends_near = upright == 1
    with jax.named_scope('norm2'):
        norm_piece(flip, 0, MROW, coef2, 1)

        @pl.when(sends_near)
        def _():
            h3_near.start()
        for r in (1, 2):
            norm_piece(r + flip, 0, FIRST, coef2, r + 1)

    wd_taps = ((1, 0), (0, NIM), (1, NIM))

    def wide_conv(dst, i, lhs_of, w_val, carry, work=None):
        s1, s2 = carry
        for m in PIECES:
            if work is not None:
                work(m)
            lhs = join(lhs_of(m))
            res = mm(lhs, w_val)
            for h in range(2):
                part = res[:, LANES * h:LANES * h + LANES]
                if dst is zo:
                    zo[h, pl.ds(i * OROW + m, CHUNK), :] = part
                else:
                    dst[h, i, pl.ds(m, CHUNK), :] = part
            r3 = res.reshape(SUB, 8, WIDE)
            s1 = s1 + sublane_sum(r3)
            s2 = s2 + sublane_sum(r3 * r3)
        return s1, s2

    def wide_stats(layer, carry):
        s1, s2 = carry
        s1, s2, finish = exchange(layer, [column_sum(s1), column_sum(s2)])
        mean, inv = moments(s1, s2, float(32 * 24 * 84))
        return mean, inv, finish

    zero = jnp.zeros((8, WIDE), F32)

    def down_lhs(slots):
        return lambda m: [yy[plane, slot, pl.ds(m + off, CHUNK), :] for slot in slots for plane, off in wd_taps]

    wd_val = wdv[...].reshape(9 * LANES, WIDE)

    def down_ahead(it):
        def work(m):
            if it == 0:
                for r in (1, 2):
                    norm_piece(r + flip, *rest(m), coef2, r + 1)
            if it < 4:
                for e in range(2):
                    norm_piece(2 * it + 3 + e + flip, m, CHUNK, coef2, 2 * it + 4 + e)
            else:
                norm_piece(LAST * upright, m, CHUNK, coef2, ROWS)
        return work

    with jax.named_scope('wide2'):
        carry = (zero, zero)
        for it in range(OLAST):
            carry = wide_conv(zo, it, down_lhs((2 * it + 1, 2 * it + 2, 2 * it + 3)), wd_val, carry, down_ahead(it))

    with jax.named_scope('halo2'):
        @pl.when(sp == 1)
        def _():
            hy0.wait_recv()
            hy1.wait_recv()

            par = load_coef(coef2)
            for m in PIECES:
                res = lone_row(m, (2,))
                for b, plane, off in ((0, 1, m), (1, 0, NIM + m)):
                    z = zo[b, pl.ds(OLAST * OROW + m, CHUNK), :] + res[:, LANES * b:LANES * b + LANES]
                    yy[plane, FAR_SLOT, pl.ds(off, CHUNK), :] = normalise(z, *par)


        @pl.when(flip == 1)
        def _():
            h3_near.wait_recv()
    with jax.named_scope('wide2B'):
        slots = (LAST + 2 * flip, ROWS, FAR_SLOT - ROWS * flip)
        carry = wide_conv(zo, OLAST, down_lhs(slots), wd_val, carry)
    mean3, inv3, fin3 = wide_stats(2, carry)
    coef3 = save_coef(2, WIDE, mean3, inv3, ndv[0:1], ndv[1:2])

    def norm3_piece(r, m, size):
        if size == 0:
            return
        step = lax.rem(r - flip + OROWS, OROWS)
        for h in range(2):
            par = load_coef(coef3, LANES * h)
            y3[r + 1, pl.ds(NIM + m, size), pl.ds(LANES * h, LANES)] = normalise(zo[h, pl.ds(pl.multiple_of(step * OROW, NIM) + m, size), :], *par)

    def norm3(r):
        norm3_piece(r, 0, OROW)

    with jax.named_scope('norm3'):
        norm3(OLAST)

        @pl.when(has_far)
        def _():
            h4_far.start()

        norm3(0)
        h4_near.start()

        @pl.loop(1, 3)
        def _(r):
            norm3_piece(r, 0, FIRST)

    def last_lhs(i, taps=(0, 1, 2)):
        return lambda m: [y3[i + p, pl.ds(m + NIM * q, CHUNK), :] for p in taps for q in range(3)]

    wb_val = wbv[...].reshape(9 * WIDE, WIDE)

    def last_ahead(it):
        def work(m):
            if it == 1:
                for r in range(1, 3):
                    norm3_piece(r, *rest(m))
                norm3_piece(3, m, CHUNK)
            elif it == 2:
                norm3_piece(4, m, CHUNK)
        return work

    with jax.named_scope('wide3A'):
        carry = (zero, zero)
        for it in (1, 2, 3, 4):
            carry = wide_conv(z_out, it, last_lhs(it), wb_val, carry, last_ahead(it))
    with jax.named_scope('wide3B'):
        with jax.named_scope('near3'):
            h4_near.wait_recv()
        carry = wide_conv(z_out, 0, last_lhs(0), wb_val, carry)
        part_w = wbv[head(2)].reshape(6 * WIDE, WIDE)
        last_w = wbv[2].reshape(3 * WIDE, WIDE)
        r = OLAST
        for m in PIECES:
            res = mm(join(last_lhs(r, (0, 1))(m)), part_w)
            z_out[0, r, pl.ds(m, CHUNK), :] = res[:, :LANES]
            z_out[1, r, pl.ds(m, CHUNK), :] = res[:, LANES:]
        with jax.named_scope('far3'):
            @pl.when(has_far)
            def _():
                h4_far.wait_recv()
        s1, s2 = carry
        for m in PIECES:
            res = mm(join(last_lhs(r, (2,))(m)), last_w)
            res = res + join([z_out[h, r, pl.ds(m, CHUNK), :] for h in range(2)])
            z_out[0, r, pl.ds(m, CHUNK), :] = res[:, :LANES]
            z_out[1, r, pl.ds(m, CHUNK), :] = res[:, LANES:]
            r3 = res.reshape(SUB, 8, WIDE)
            s1 = s1 + sublane_sum(r3)
            s2 = s2 + sublane_sum(r3 * r3)
        carry = s1, s2
    mean4, inv4, fin4 = wide_stats(3, carry)
    for k, v in enumerate((mean4, inv4, nbv[0, 0:1], nbv[0, 1:2])):
        c_out[k:k + 1] = v

    with jax.named_scope('drain'):
        hx_near.wait_send()
        h4_near.wait_send()

        @pl.when(has_far)
        def _():
            hx_far.wait_send()
            h4_far.wait_send()

        @pl.when(sends_near)
        def _():
            h3_near.wait_send()

        @pl.when(sp == 2)
        def _():
            hy0.wait_send()
            hy1.wait_send()
        for f in (fin1, fin2, fin3, fin4):
            f()


def result_kernel(z_ref, c_ref, out_ref, yo, cf, sem):
    flip = 1 - lax.rem(lax.axis_index("sp"), 2)

    def copy(r):
        return pltpu.make_async_copy(yo.at[r], out_ref.at[r + flip * (OLAST - 2 * r)], sem.at[r])

    mean, inv, gamma, beta = [c_ref[k:k + 1] for k in range(4)]
    scale = gamma * inv
    cf[0:1] = scale
    cf[1:2] = beta - mean * scale
    small = jnp.logical_and(jnp.max(jnp.abs(scale)) < 1e15, jnp.max(jnp.abs(mean)) < 1e20)

    @pl.when(small)
    def _():
        @pl.loop(0, OROWS)
        def _(r):
            for h in range(2):
                lanes = pl.ds(LANES * h, LANES)
                y = z_ref[h, r] * cf[0:1, lanes] + cf[1:2, lanes]
                yo[r, :, lanes] = jnp.maximum(y, 0.0).astype(BF16)
            copy(r).start()

    @pl.when(jnp.logical_not(small))
    def _():
        @pl.loop(0, OROWS)
        def _(r):
            for h in range(2):
                lanes = pl.ds(LANES * h, LANES)
                mean, inv, gamma, beta = [c_ref[k:k + 1, lanes] for k in range(4)]
                yo[r, :, lanes] = jnp.maximum(gamma * (z_ref[h, r] - mean) * inv + beta, 0.0).astype(BF16)
            copy(r).start()

    @pl.loop(0, OROWS)
    def _(r):
        copy(r).wait()


def solution(mesh):
    any_spec = pl.BlockSpec(memory_space=pl.ANY)
    dma = pltpu.SemaphoreType.DMA

    def local_stack(images, w_a, norm_a, w_down, norm_down, w_b, norm_b):
        z_last, coef = pl.pallas_call(
            kernel,
            out_shape=(pltpu.VMEM((2, OROWS, OROW, LANES), F32), pltpu.VMEM((8, WIDE), F32)),
            in_specs=[any_spec] * 7,
            out_specs=(pl.BlockSpec(memory_space=pltpu.VMEM),) * 2,
            scratch_shapes=[
                pltpu.VMEM((12, NIM, COLS, LANES), BF16),
                pltpu.VMEM((2, ROWS + 2, YROW, LANES), BF16),
                pltpu.VMEM((2, ROWS, MROW, LANES), F32),
                pltpu.VMEM((2, OROWS * OROW, LANES), F32),
                pltpu.VMEM((OROWS + 2, O3ROW, WIDE), BF16),
                pltpu.VMEM((2, YROW, LANES), BF16),
                pltpu.VMEM((2, YROW, LANES), BF16),
                pltpu.VMEM((512, WIDE), BF16),
                pltpu.VMEM((2, 1792, WIDE), BF16),
                pltpu.VMEM((3, 3, LANES, WIDE), BF16),
                pltpu.VMEM((3, 3, WIDE, WIDE), BF16),
                pltpu.VMEM((2, 2, LANES), F32),
                pltpu.VMEM((2, WIDE), F32),
                pltpu.VMEM((1, 2, WIDE), F32),
                pltpu.VMEM((4, 8, WIDE), F32),
                pltpu.VMEM((2, 1, WIDE), F32),
                pltpu.VMEM((2, GROUPS, 1, WIDE), F32),
                pltpu.VMEM((2, 1, 512), F32),
                pltpu.VMEM((2, GROUPS, 1, 512), F32),
                dma((ROWS,)), dma((15,)),
                *[dma((2,))] * 4, *[dma((3,))] * 2, *[dma((2,))] * 2,
                *[dma((4, GROUPS))] * 2,
            ],
            compiler_params=pltpu.CompilerParams(
                collective_id=0, has_side_effects=True, vmem_limit_bytes=VLIM),
        )(images, w_a.reshape(2, 3, 384, LANES), norm_a, w_down, norm_down, w_b.reshape(3, 3, WIDE, WIDE), norm_b)
        out = pl.pallas_call(
            result_kernel,
            out_shape=jax.ShapeDtypeStruct((OROWS, OROW, WIDE), BF16),
            in_specs=[pl.BlockSpec(memory_space=pltpu.VMEM)] * 2,
            out_specs=any_spec,
            scratch_shapes=[pltpu.VMEM((OROWS, OROW, WIDE), BF16), pltpu.VMEM((8, WIDE), F32), dma((OROWS,))],
            compiler_params=pltpu.CompilerParams(vmem_limit_bytes=6 * 1024 * 1024),
        )(z_last, coef)
        return jnp.transpose(out.reshape(OROWS, OCOLS, NIM, WIDE), (2, 0, 1, 3))

    act_spec = P(('pod', 'dp'), 'sp', None, None)
    return jax.shard_map(local_stack, mesh=mesh, in_specs=(act_spec, P(), P(), P(), P(), P(), P()), out_specs=act_spec, check_vma=False)
```
